32 devices in a mesh: dp: 8 (over z, core), tensor: 4 (over y, x).
Axes of the slice: x: 2, y: 2, z: 4, core: 2. Of those that a mesh axis runs over, the one named last changes fastest.
Arguments:
- hidden: bfloat16 [2048, 8, 1536], P('tensor', 'dp'), may hold values from -6 to 6
- cotangent: bfloat16 [2048, 8, 1536], P('tensor', 'dp'), may hold values from -6 to 6
- input_gain: float32 [1536], replicated, may hold values from 0.5 to 1.5
- inner_weight: float32 [2, 1536, 3072], P(None, 'dp', 'tensor'), may hold values from -0.15625 to 0.15625
- step_weight: float32 [1536, 48], P('dp', 'tensor'), may hold values from -0.15625 to 0.15625
- state_weight: float32 [1536, 256], P(('dp', 'tensor')), may hold values from -0.15625 to 0.15625
- inner_taps: float32 [5, 3072], P(None, 'tensor'), may hold values from -3 to 3
- state_taps: float32 [5, 256], replicated, may hold values from -3 to 3
- head_params: float32 [3, 48], P(None, 'tensor'), may hold values from -7 to 3, as said below
- gated_gain: float32 [3072], P('tensor'), may hold values from 0.5 to 1.5
- output_matrix: float32 [3072, 1536], P('tensor', 'dp'), may hold values from -0.109375 to 0.109375
- first_input_gain: float32 [1536], replicated, may hold values from -6 to 6
- first_inner_weight: float32 [2, 1536, 3072], P(None, 'dp', 'tensor'), may hold values from -6 to 6
- first_step_weight: float32 [1536, 48], P('dp', 'tensor'), may hold values from -6 to 6
- first_state_weight: float32 [1536, 256], P(('dp', 'tensor')), may hold values from -6 to 6
- first_inner_taps: float32 [5, 3072], P(None, 'tensor'), may hold values from -6 to 6
- first_state_taps: float32 [5, 256], replicated, may hold values from -6 to 6
- first_head_params: float32 [3, 48], P(None, 'tensor'), may hold values from -6 to 6
- first_gated_gain: float32 [3072], P('tensor'), may hold values from -6 to 6
- first_output_weight: float32 [3072, 1536], P('tensor', 'dp'), may hold values from -6 to 6
- second_input_gain: float32 [1536], replicated, may hold values from 1 to 163
- second_inner_weight: float32 [2, 1536, 3072], P(None, 'dp', 'tensor'), may hold values from 1 to 163
- second_step_weight: float32 [1536, 48], P('dp', 'tensor'), may hold values from 1 to 163
- second_state_weight: float32 [1536, 256], P(('dp', 'tensor')), may hold values from 1 to 163
- second_inner_taps: float32 [5, 3072], P(None, 'tensor'), may hold values from 1 to 163
- second_state_taps: float32 [5, 256], replicated, may hold values from 1 to 163
- second_head_params: float32 [3, 48], P(None, 'tensor'), may hold values from 1 to 163
- second_gated_gain: float32 [3072], P('tensor'), may hold values from 1 to 163
- second_output_weight: float32 [3072, 1536], P('tensor', 'dp'), may hold values from 1 to 163
Outputs:
- result: bfloat16 [2048, 8, 1536], P('tensor', 'dp')
- gradient_hidden: float32 [2048, 8, 1536], P('tensor', 'dp')
- gradient_input_gain: float32 [1536], replicated
- gradient_inner_weight: float32 [2, 1536, 3072], P(None, 'dp', 'tensor')
- step_weight_gradient: float32 [1536, 48], P('dp', 'tensor')
- gradient_state_weight: float32 [1536, 256], P(('dp', 'tensor'))
- gradient_inner_taps: float32 [5, 3072], P(None, 'tensor')
- gradient_state_taps: float32 [5, 256], replicated
- gradient_head_params: float32 [3, 48], P(None, 'tensor')
- gradient_gated_gain: float32 [3072], P('tensor')
- gradient_output_weight: float32 [3072, 1536], P('tensor', 'dp')
- updated_input_gain: float32 [1536], replicated
- updated_inner_weight: float32 [2, 1536, 3072], P(None, 'dp', 'tensor')
- updated_step_weight: float32 [1536, 48], P('dp', 'tensor')
- updated_state_weight: float32 [1536, 256], P(('dp', 'tensor'))
- updated_inner_taps: float32 [5, 3072], P(None, 'tensor')
- updated_state_taps: float32 [5, 256], replicated
- updated_head_params: float32 [3, 48], P(None, 'tensor')
- updated_gated_gain: float32 [3072], P('tensor')
- updated_output_weight: float32 [3072, 1536], P('tensor', 'dp')
- updated_first_input_gain: float32 [1536], replicated
- updated_first_inner_weight: float32 [2, 1536, 3072], P(None, 'dp', 'tensor')
- updated_first_step_weight: float32 [1536, 48], P('dp', 'tensor')
- updated_first_state_weight: float32 [1536, 256], P(('dp', 'tensor'))
- updated_first_inner_taps: float32 [5, 3072], P(None, 'tensor')
- updated_first_state_taps: float32 [5, 256], replicated
- updated_first_head_params: float32 [3, 48], P(None, 'tensor')
- updated_first_gated_gain: float32 [3072], P('tensor')
- updated_first_output_weight: float32 [3072, 1536], P('tensor', 'dp')
- updated_second_input_gain: float32 [1536], replicated
- updated_second_inner_weight: float32 [2, 1536, 3072], P(None, 'dp', 'tensor')
- updated_second_step_weight: float32 [1536, 48], P('dp', 'tensor')
- updated_second_state_weight: float32 [1536, 256], P(('dp', 'tensor'))
- updated_second_inner_taps: float32 [5, 3072], P(None, 'tensor')
- updated_second_state_taps: float32 [5, 256], replicated
- updated_second_head_params: float32 [3, 48], P(None, 'tensor')
- updated_second_gated_gain: float32 [3072], P('tensor')
- updated_second_output_weight: float32 [3072, 1536], P('tensor', 'dp')
The draws below stay inside these ranges and needn't reach their ends.
Inputs may be any that keep to these rules, and one draw needn't show every extreme that they name: Row 0 of head_params lies in [-1, 2.8), row 1 in [-7, -2), row 2 in [0.5, 1.5).
All inputs are finite; a program needn't handle non-finite values.
Results may differ from the reference program's by a relative error of at most 0.01.
The reference program's roundings to bfloat16 on the way count: a program that leaves them out, or rounds other values in their place, can miss the bound.
Values may be sent and summed in bfloat16 or wider, within the bound.
A program may use at most 256 MiB of HBM per device.

```python
import math
import jax
import jax.numpy as jnp
from jax import lax

D = 1536
H = 48
N = 128
K = 4
GROUP = 256
LEN = 2048
INNER = 3072
SEQS = 8
TOKENS = 16384


def draw_head_params(key, part):
    key_log = jax.random.fold_in(key, 11)
    key_bias = jax.random.fold_in(key, 12)
    key_skip = jax.random.fold_in(key, 13)
    a_log = jax.random.uniform(key_log, (H,), jnp.float32, -1.0, 2.8)
    dt_bias = jax.random.uniform(key_bias, (H,), jnp.float32, -7.0, -2.0)
    skip_gain = jax.random.uniform(key_skip, (H,), jnp.float32, 0.5, 1.5)
    return jnp.stack([a_log, dt_bias, skip_gain])


def level_of(own_key, dims, cuts, smallest, high):
    level = 1.0
    for position, blocks in cuts:
        draws = jax.random.uniform(jax.random.fold_in(jax.random.fold_in(own_key, 6), position), (blocks,), jnp.float32, smallest / len(cuts), high / len(cuts))
        level = level * jnp.repeat(jnp.exp(draws), dims[position] // blocks).reshape((-1,) + (1,) * (len(dims) - 1 - position))
    return level


def normal_values(stream_key, extent, scale, bound, cuts=(), dtype=jnp.bfloat16):
    gain = level_of(stream_key, extent, cuts, -0.22, 0.18) if cuts else 1.0
    values = jax.random.normal(stream_key, extent, jnp.float32) * scale * gain
    return jnp.minimum(jnp.maximum(values, -bound), bound).astype(dtype)


def setup_inputs(seed: int = 0) -> dict:
    arg_keys = jax.random.split(jax.random.key(seed), 30)
    hidden = normal_values(arg_keys[0], (LEN, SEQS, D), 1.0, 6.0, ((0, 4), (1, 8)))
    cotangent = normal_values(arg_keys[1], (LEN, SEQS, D), 1.0, 6.0, ((0, 4), (1, 8)))
    input_gain = jnp.clip(1.0 + 0.1 * jax.random.normal(arg_keys[2], (D,), jnp.float32), 0.5, 1.5)
    inner_weight = normal_values(arg_keys[3], (2, D, INNER), D ** -0.5, 0.15625, ((1, 8), (2, 4)), jnp.float32)
    step_weight = normal_values(arg_keys[4], (D, H), D ** -0.5, 0.15625, ((0, 8), (1, 4)), jnp.float32)
    state_weight = normal_values(arg_keys[5], (D, 2 * N), D ** -0.5, 0.15625, ((0, 32),), jnp.float32)
    inner_taps = normal_values(arg_keys[6], (K + 1, INNER), K ** -0.5, 3.0, ((1, 4),), jnp.float32)
    state_taps = normal_values(arg_keys[7], (K + 1, 2 * N), K ** -0.5, 3.0, (), jnp.float32)
    head_params = draw_head_params(jax.random.fold_in(arg_keys[29], 71), 0)
    gated_gain = jnp.clip(1.0 + 0.1 * jax.random.normal(arg_keys[9], (INNER,), jnp.float32), 0.5, 1.5)
    output_matrix = normal_values(arg_keys[10], (INNER, D), INNER ** -0.5, 0.109375, ((0, 4), (1, 8)), jnp.float32)
    first_input_gain = normal_values(arg_keys[11], (D,), (max(1, TOKENS // 13000)), 6.0, (), jnp.float32)
    first_inner_weight = normal_values(arg_keys[12], (2, D, INNER), (max(1, TOKENS // 13000)), 6.0, ((1, 8), (2, 4)), jnp.float32)
    first_step_weight = normal_values(arg_keys[13], (D, H), (max(1, TOKENS // 13000)), 6.0, ((0, 8), (1, 4)), jnp.float32)
    first_state_weight = normal_values(arg_keys[14], (D, 2 * N), (max(1, TOKENS // 13000)), 6.0, ((0, 32),), jnp.float32)
    first_inner_taps = normal_values(arg_keys[15], (K + 1, INNER), (max(1, TOKENS // 13000)), 6.0, ((1, 4),), jnp.float32)
    first_state_taps = normal_values(arg_keys[16], (K + 1, 2 * N), (max(1, TOKENS // 13000)), 6.0, (), jnp.float32)
    first_head_params = normal_values(arg_keys[17], (3, H), (max(1, TOKENS // 13000)), 6.0, ((1, 4),), jnp.float32)
    first_gated_gain = normal_values(arg_keys[18], (INNER,), (max(1, TOKENS // 13000)), 6.0, ((0, 4),), jnp.float32)
    first_output_weight = normal_values(arg_keys[19], (INNER, D), (max(1, TOKENS // 13000)), 6.0, ((0, 4), (1, 8)), jnp.float32)
    second_input_gain = jnp.clip(jnp.exp(jax.random.uniform(arg_keys[20], (D,), jnp.float32, math.log(1.0), math.log(163.0))), 1.0, 163.0)
    second_inner_weight = jnp.clip(jnp.exp(math.log(163.0) - 5.09375 * jax.random.uniform(arg_keys[21], (2, D, INNER), jnp.float32) ** level_of(arg_keys[21], (2, D, INNER), ((1, 8), (2, 4)), -0.2, 0.2)), 1.0, 163.0)
    second_step_weight = jnp.clip(jnp.exp(math.log(163.0) - 5.09375 * jax.random.uniform(arg_keys[22], (D, H), jnp.float32) ** level_of(arg_keys[22], (D, H), ((0, 8), (1, 4)), -0.2, 0.2)), 1.0, 163.0)
    second_state_weight = jnp.clip(jnp.exp(math.log(163.0) - 5.09375 * jax.random.uniform(arg_keys[23], (D, 2 * N), jnp.float32) ** level_of(arg_keys[23], (D, 2 * N), ((0, 32),), -0.2, 0.2)), 1.0, 163.0)
    second_inner_taps = jnp.clip(jnp.exp(math.log(163.0) - 5.09375 * jax.random.uniform(arg_keys[24], (K + 1, INNER), jnp.float32) ** level_of(arg_keys[24], (K + 1, INNER), ((1, 4),), -0.2, 0.2)), 1.0, 163.0)
    second_state_taps = jnp.clip(jnp.exp(jax.random.uniform(arg_keys[25], (K + 1, 2 * N), jnp.float32, math.log(1.0), math.log(163.0))), 1.0, 163.0)
    second_head_params = jnp.clip(jnp.exp(math.log(163.0) - 5.09375 * jax.random.uniform(arg_keys[26], (3, H), jnp.float32) ** level_of(arg_keys[26], (3, H), ((1, 4),), -0.2, 0.2)), 1.0, 163.0)
    second_gated_gain = jnp.clip(jnp.exp(math.log(163.0) - 5.09375 * jax.random.uniform(arg_keys[27], (INNER,), jnp.float32) ** level_of(arg_keys[27], (INNER,), ((0, 4),), -0.2, 0.2)), 1.0, 163.0)
    second_output_weight = jnp.clip(jnp.exp(math.log(163.0) - 5.09375 * jax.random.uniform(arg_keys[28], (INNER, D), jnp.float32) ** level_of(arg_keys[28], (INNER, D), ((0, 4), (1, 8)), -0.2, 0.2)), 1.0, 163.0)
    return dict(hidden=hidden, cotangent=cotangent, input_gain=input_gain, inner_weight=inner_weight, step_weight=step_weight, state_weight=state_weight, inner_taps=inner_taps, state_taps=state_taps, head_params=head_params, gated_gain=gated_gain, output_matrix=output_matrix, first_input_gain=first_input_gain, first_inner_weight=first_inner_weight, first_step_weight=first_step_weight, first_state_weight=first_state_weight, first_inner_taps=first_inner_taps, first_state_taps=first_state_taps, first_head_params=first_head_params, first_gated_gain=first_gated_gain, first_output_weight=first_output_weight, second_input_gain=second_input_gain, second_inner_weight=second_inner_weight, second_step_weight=second_step_weight, second_state_weight=second_state_weight, second_inner_taps=second_inner_taps, second_state_taps=second_state_taps, second_head_params=second_head_params, second_gated_gain=second_gated_gain, second_output_weight=second_output_weight)


norm_eps = 1e-05
beta_first = 0.9
beta_second = 0.95
adam_eps = 1e-08
decay_rate = 0.1
step_count = 4.0
rates = (0.2, 0.008, 0.008, 0.008, 0.1, 0.1, 0.4, 0.2, 0.006)
precise_setting = lax.Precision.HIGHEST

def contract_last(values, weight):
    return lax.dot_general(values, weight, (((1,), (1,)), ((), ())), preferred_element_type=jnp.float32)

def contract_first(left, right):
    return lax.dot_general(left, right, (((0,), (0,)), ((), ())), preferred_element_type=jnp.float32)

def conv_silu(values, taps):
    length = values.shape[0]
    width = taps.shape[0] - 1
    padded = jnp.pad(values, ((width - 1, 0), (0, 0), (0, 0)))
    total = jnp.broadcast_to(taps[width], values.shape)
    for offset in range(width):
        total = total + taps[offset] * padded[offset:offset + length]
    return jax.nn.silu(total)

def group_step(state, block):
    inputs, steps, logs, key_rows, query_rows = block
    cumul = jnp.cumsum(logs, axis=0)
    score_matrix = jnp.einsum('dtv,htv->dht', query_rows, key_rows, precision=precise_setting)
    count = logs.shape[0]
    causal = (jnp.arange(count)[:, None] >= jnp.arange(count)[None, :])[:, :, None, None]
    spread = jnp.where(causal, cumul[:, None] - cumul[None, :], 0.0)
    mixing = jnp.where(causal, jnp.exp(spread), 0.0) * score_matrix[..., None] * steps[None]
    inner_part = jnp.einsum('qksh,kshp->qshp', mixing, inputs, precision=precise_setting)
    carried = jnp.einsum('qsn,shnp->qshp', query_rows, state, precision=precise_setting) * jnp.exp(cumul)[..., None]
    final = cumul[-1]
    weights = jnp.exp(final[None] - cumul) * steps
    update = jnp.einsum('ksn,kshp->shnp', key_rows, weights[..., None] * inputs, precision=precise_setting)
    return (jnp.exp(final)[..., None, None] * state + update, inner_part + carried)

def scan_heads(inputs, steps, logs, key_rows, query_rows):
    length, seqs, heads, size = inputs.shape
    blocks = length // GROUP

    def split(values):
        return values.reshape((blocks, GROUP) + values.shape[1:])
    start = jnp.zeros((seqs, heads, key_rows.shape[-1], size), jnp.float32)
    final_state, outputs = lax.scan(jax.checkpoint(group_step), start, (split(inputs), split(steps), split(logs), split(key_rows), split(query_rows)))
    return outputs.reshape(inputs.shape)

def mixer(inner_pre, state_pre, step_pre, gate_pre, inner_taps, state_taps, head_params):
    length, seqs, width = inner_pre.shape
    heads = step_pre.shape[-1]
    half_state = state_pre.shape[-1] // 2
    inner_act = conv_silu(inner_pre, inner_taps).reshape(length, seqs, heads, width // heads)
    state_act = conv_silu(state_pre, state_taps)
    steps = jax.nn.softplus(step_pre + head_params[1])
    logs = -jnp.exp(head_params[0]) * steps
    scanned = scan_heads(inner_act, steps, logs, state_act[..., :half_state], state_act[..., half_state:])
    mixed = scanned + head_params[2][:, None] * inner_act
    return mixed.reshape(length, seqs, width) * jax.nn.silu(gate_pre)

def adam_step(param, first, second_moment, grad, rate):
    first_new = beta_first * first + (1.0 - beta_first) * grad
    second_new = beta_second * second_moment + (1.0 - beta_second) * grad * grad
    first_hat = first_new / (1.0 - beta_first ** step_count)
    second_hat = second_new / (1.0 - beta_second ** step_count)
    moved = param - rate * (first_hat / (jnp.sqrt(second_hat) + adam_eps) + decay_rate * param)
    return (moved, first_new, second_new)

def reference(hidden, cotangent, input_gain, inner_weight, step_weight, state_weight, inner_taps, state_taps, head_params, gated_gain, output_matrix, first_input_gain, first_inner_weight, first_step_weight, first_state_weight, first_inner_taps, first_state_taps, first_head_params, first_gated_gain, first_output_weight, second_input_gain, second_inner_weight, second_step_weight, second_state_weight, second_inner_taps, second_state_taps, second_head_params, second_gated_gain, second_output_weight):
    params = (input_gain, inner_weight, step_weight, state_weight, inner_taps, state_taps, head_params, gated_gain, output_matrix)
    firsts = (first_input_gain, first_inner_weight, first_step_weight, first_state_weight, first_inner_taps, first_state_taps, first_head_params, first_gated_gain, first_output_weight)
    seconds = (second_input_gain, second_inner_weight, second_step_weight, second_state_weight, second_inner_taps, second_state_taps, second_head_params, second_gated_gain, second_output_weight)
    inner_b = inner_weight.astype(jnp.bfloat16)
    step_b = step_weight.astype(jnp.bfloat16)
    state_b = state_weight.astype(jnp.bfloat16)
    output_b = output_matrix.astype(jnp.bfloat16)

    def per_sequence(totals, pair):
        rows_in, row_cotangents = pair
        length = rows_in.shape[0]
        base = rows_in.astype(jnp.float32)[:, None, :]
        rstd = lax.rsqrt(lax.optimization_barrier(jnp.mean(base * base, -1, keepdims=True)) + norm_eps)
        normed = base * rstd
        flat_in = (normed * input_gain).astype(jnp.bfloat16).reshape(length, -1)

        def project(weight):
            return jnp.dot(flat_in, weight, preferred_element_type=jnp.float32).reshape(length, 1, weight.shape[1])
        gate_pre = project(inner_b[0])
        inner_pre = project(inner_b[1])
        step_pre = project(step_b)
        state_pre = project(state_b)
        gated, pullback = jax.vjp(mixer, inner_pre, state_pre, step_pre, gate_pre, inner_taps, state_taps, head_params)
        scale = lax.rsqrt(lax.optimization_barrier(jnp.mean(gated * gated, -1, keepdims=True)) + norm_eps)
        unit = gated * scale
        normed_out = (unit * gated_gain).astype(jnp.bfloat16).reshape(length, -1)
        branch = jnp.dot(normed_out, output_b, preferred_element_type=jnp.float32)
        result_rows = (base[:, 0] + branch).astype(jnp.bfloat16)
        d_normed = contract_last(row_cotangents, output_b).reshape(length, 1, -1)
        grad_output = contract_first(normed_out, row_cotangents)
        grad_gated_gain = lax.optimization_barrier(jnp.sum(d_normed * unit, (0, 1)))
        d_unit = d_normed * gated_gain
        d_gated = scale * (d_unit - unit * lax.optimization_barrier(jnp.mean(d_unit * unit, -1, keepdims=True)))
        d_inner_pre, d_state_pre, d_step_pre, d_gate_pre, grad_inner_taps, grad_state_taps, grad_head = pullback(d_gated)

        def flatten(values):
            return values.reshape(length, values.shape[-1]).astype(jnp.bfloat16)
        gate_flat = flatten(d_gate_pre)
        inner_flat = flatten(d_inner_pre)
        step_flat = flatten(d_step_pre)
        state_flat = flatten(d_state_pre)
        grad_inner = jnp.stack([contract_first(flat_in, gate_flat), contract_first(flat_in, inner_flat)])
        grad_step = contract_first(flat_in, step_flat)
        grad_state = contract_first(flat_in, state_flat)
        d_in = (contract_last(gate_flat, inner_b[0]) + contract_last(inner_flat, inner_b[1]) + contract_last(step_flat, step_b) + contract_last(state_flat, state_b))[:, None, :]
        grad_input_gain = lax.optimization_barrier(jnp.sum(d_in * normed, (0, 1)))
        d_hat = d_in * input_gain
        grad_rows = row_cotangents.astype(jnp.float32)[:, None, :] + rstd * (d_hat - normed * lax.optimization_barrier(jnp.mean(d_hat * normed, -1, keepdims=True)))
        pieces = (grad_input_gain, grad_inner, grad_step, grad_state, grad_inner_taps, grad_state_taps, grad_head, grad_gated_gain, grad_output)
        totals = tuple((summed + piece for summed, piece in zip(totals, pieces)))
        return (totals, (result_rows, grad_rows[:, 0]))
    zeros = tuple((jnp.zeros(param.shape, jnp.float32) for param in params))
    grads, (results, grad_seqs) = lax.scan(per_sequence, zeros, (hidden.transpose(1, 0, 2), cotangent.transpose(1, 0, 2)))
    result = results.transpose(1, 0, 2)
    gradient_hidden = grad_seqs.transpose(1, 0, 2)
    stepped = [adam_step(param, first, second_moment, grad, rate) for param, first, second_moment, grad, rate in zip(params, firsts, seconds, grads, rates)]
    moved = [entry[0] for entry in stepped]
    first_new = [entry[1] for entry in stepped]
    second_new = [entry[2] for entry in stepped]
    return (result, gradient_hidden, *grads, *moved, *first_new, *second_new)
```

```python
import functools
import jax
import jax.numpy as jnp
from jax import lax
from jax.experimental import pallas as pl
from jax.experimental.pallas import tpu as pltpu
from jax.sharding import PartitionSpec as P

GROUP = 256
norm_eps = 1e-05
beta_first = 0.9
beta_second = 0.95
adam_eps = 1e-08
decay_rate = 0.1
step_count = 4.0
rates = (0.2, 0.008, 0.008, 0.008, 0.1, 0.1, 0.4, 0.2, 0.006)

LANES = 128
CARRY = 8
BLOCKED = -1e30
f32 = jnp.float32
bf16 = jnp.bfloat16


def mm(a, b):
    return lax.dot_general(a, b, (((1,), (0,)), ((), ())), preferred_element_type=f32)


def mm_nt(a, b):
    return lax.dot_general(a, b, (((1,), (1,)), ((), ())), preferred_element_type=f32)


def mm_exact(a, b):
    return lax.dot_general(
        a, b, (((1,), (0,)), ((), ())), precision=lax.Precision.HIGHEST, preferred_element_type=f32
    )


def mm_split(values, weight):
    high = values.astype(bf16)
    low = (values - high.astype(f32)).astype(bf16)
    return mm(high, weight) + mm(low, weight)


def sigmoid(v):
    return 1.0 / (1.0 + jnp.exp(-v))


def tri_lower(count):
    rows = lax.broadcasted_iota(jnp.int32, (count, count), 0)
    cols = lax.broadcasted_iota(jnp.int32, (count, count), 1)
    return rows >= cols


def step_terms(step_pre, heads_ref):
    shifted = step_pre + heads_ref[1:2, :]
    steps = jnp.maximum(shifted, 0.0) + jnp.log1p(jnp.exp(-jnp.abs(shifted)))
    logs = heads_ref[0:1, :] * steps
    count = logs.shape[0]
    cumul = mm_exact(tri_lower(count).astype(f32), logs)
    return shifted, steps, logs, cumul


def forward_kernel(
    width, size, pre_ref, taps_ref, heads_ref, skip_ref, spread_ref,
    scanned_ref, conv_ref, gated_ref, squares_ref, states_ref,
    ext, state, act,
):
    count = pre_ref.shape[0]
    half = count // 2
    conv_width = taps_ref.shape[1]
    taps = taps_ref.shape[0] - 1
    state_size = (conv_width - width) // 2
    per_tile = LANES // size

    @pl.when(pl.program_id(1) == 0)
    def _():
        ext[0:CARRY, :] = jnp.zeros((CARRY, conv_width), f32)
        state[...] = jnp.zeros_like(state)

    states_ref[0] = state[...]
    for start in range(0, conv_width, LANES):
        cols = slice(start, start + LANES)
        ext[CARRY : CARRY + count, cols] = pre_ref[:, width + start : width + start + LANES]
        total = taps_ref[taps : taps + 1, cols]
        for j in range(taps):
            total = total + taps_ref[j : j + 1, cols] * ext[CARRY + 1 - taps + j : CARRY + 1 - taps + j + count, cols]
        conv_ref[:, cols] = total
        act[:, cols] = total * sigmoid(total)
        ext[0:CARRY, cols] = ext[count : count + CARRY, cols]

    shifted, steps, logs, cumul = step_terms(pre_ref[:, width + conv_width :], heads_ref)
    cumul_t = cumul.T
    final = cumul[count - 1 : count, :]
    decay_in = jnp.exp(cumul)
    decay_out = jnp.exp(final - cumul)
    keys = act[:, width : width + state_size].astype(bf16)
    queries = act[:, width + state_size :].astype(bf16)
    keys_t = act[:, width : width + state_size].T.astype(bf16)
    scores = mm_nt(queries, keys)
    causal = tri_lower(half)
    lane = lax.broadcasted_iota(jnp.int32, (count, LANES), 1)
    squares = jnp.zeros((count, LANES), f32)
    for tile in range(width // LANES):
        cols = slice(tile * LANES, (tile + 1) * LANES)
        spread = spread_ref[:, cols]
        inner = act[:, cols]
        scaled = inner * mm_split(steps, spread)
        scaled_b = scaled.astype(bf16)
        mixed = None
        for k in range(per_tile):
            head = tile * per_tile + k
            col = cumul[:, head : head + 1]
            row = cumul_t[head : head + 1, :]
            first = jnp.exp(jnp.where(causal, col[:half] - row[:, :half], BLOCKED)) * scores[:half, :half]
            low = jnp.exp(col[half:] - row[:, :half]) * scores[half:, :half]
            last = jnp.exp(jnp.where(causal, col[half:] - row[:, half:], BLOCKED)) * scores[half:, half:]
            top = mm(first.astype(bf16), scaled_b[:half])
            bottom = mm(jnp.concatenate([low.astype(bf16), last.astype(bf16)], axis=1), scaled_b)
            part = jnp.concatenate([top, bottom], axis=0)
            mixed = part if mixed is None else jnp.where(lane >= k * size, part, mixed)
        in_wide = mm_split(decay_in, spread)
        out_wide = mm_split(decay_out, spread)
        held = state[:, cols]
        scanned = mixed + in_wide * mm(queries, held.astype(bf16))
        state[:, cols] = in_wide[count - 1 : count, :] * held + mm(keys_t, (out_wide * scaled).astype(bf16))
        scanned_ref[:, cols] = scanned
        gate = pre_ref[:, cols]
        gated = (scanned + skip_ref[:, cols] * inner) * (gate * sigmoid(gate))
        gated_ref[:, cols] = gated
        squares = squares + gated * gated
    squares_ref[...] = jnp.sum(squares, axis=1, keepdims=True)


def backward_kernel(
    width, size, pre_ref, conv_ref, scanned_ref, dnormed_ref, token_ref, states_ref,
    taps_ref, heads_ref, skip_ref, gain_ref, spread_ref, gather_ref,
    dpre_ref, taps_grad_ref, wide_grad_ref, heads_grad_ref,
    ext, dstate, dscores, in_rows, out_rows, dstate_b, finals,
):
    count = pre_ref.shape[0]
    half = count // 2
    conv_width = taps_ref.shape[1]
    taps = taps_ref.shape[0] - 1
    state_size = (conv_width - width) // 2
    per_tile = LANES // size

    @pl.when(pl.program_id(1) == 0)
    def _():
        ext[count : count + CARRY, :] = jnp.zeros((CARRY, conv_width), f32)
        dstate[...] = jnp.zeros_like(dstate)

    @pl.when((pl.program_id(0) == 0) & (pl.program_id(1) == 0))
    def _():
        taps_grad_ref[...] = jnp.zeros_like(taps_grad_ref)
        wide_grad_ref[...] = jnp.zeros_like(wide_grad_ref)
        heads_grad_ref[...] = jnp.zeros_like(heads_grad_ref)

    shifted, steps, logs, cumul = step_terms(pre_ref[:, width + conv_width :], heads_ref)
    cumul_t = cumul.T
    final = cumul[count - 1 : count, :]
    decay_in = jnp.exp(cumul)
    decay_out = jnp.exp(final - cumul)
    key_cols = slice(width, width + state_size)
    query_cols = slice(width + state_size, conv_width)
    key_pre = conv_ref[:, key_cols]
    query_pre = conv_ref[:, query_cols]
    key_sig = sigmoid(key_pre)
    query_sig = sigmoid(query_pre)
    keys = (key_pre * key_sig).astype(bf16)
    queries = (query_pre * query_sig).astype(bf16)
    queries_t = (query_pre * query_sig).T.astype(bf16)
    scores_t = mm_nt(keys, queries)
    rows = lax.broadcasted_iota(jnp.int32, (half, half), 0)
    columns = lax.broadcasted_iota(jnp.int32, (half, half), 1)
    causal_t = columns >= rows
    lane = lax.broadcasted_iota(jnp.int32, (count, LANES), 1)
    dscores[...] = jnp.zeros_like(dscores)
    scale = token_ref[:, 0:1]
    pull = token_ref[:, 1:2]
    dcumul = jnp.zeros((count, LANES), f32)
    dsteps = jnp.zeros((count, LANES), f32)
    for tile in range(width // LANES):
        cols = slice(tile * LANES, (tile + 1) * LANES)
        spread = spread_ref[:, cols]
        gather = gather_ref[cols, :]
        conv = conv_ref[:, cols]
        sig = sigmoid(conv)
        inner = conv * sig
        gate = pre_ref[:, cols]
        gate_sig = sigmoid(gate)
        gate_act = gate * gate_sig
        scanned = scanned_ref[:, cols]
        mixed = scanned + skip_ref[:, cols] * inner
        gated = mixed * gate_act
        dnormed = dnormed_ref[:, cols]
        wide_grad_ref[0:1, cols] += jnp.sum(dnormed * gated * scale, axis=0, keepdims=True)
        dgated = scale * (dnormed * gain_ref[:, cols]) - pull * gated
        dmixed = dgated * gate_act
        dgate = dgated * mixed * (gate_sig * (1.0 + gate * (1.0 - gate_sig)))
        dpre_ref[:, cols] = dgate.astype(bf16)
        wide_grad_ref[1:2, cols] += jnp.sum(dmixed * inner, axis=0, keepdims=True)
        dmixed_b = dmixed.astype(bf16)
        steps_wide = mm_split(steps, spread)
        scaled = inner * steps_wide
        scaled_b = scaled.astype(bf16)
        dscaled = None
        for k in range(per_tile):
            head = tile * per_tile + k
            col = cumul[:, head : head + 1]
            row = cumul_t[head : head + 1, :]
            own = jnp.where((lane >= k * size) & (lane < (k + 1) * size), scaled, 0.0).astype(bf16)
            first = jnp.exp(jnp.where(causal_t, row[:, :half] - col[:half], BLOCKED))
            right = jnp.exp(row[:, half:] - col[:half])
            last = jnp.exp(jnp.where(causal_t, row[:, half:] - col[half:], BLOCKED))
            top = mm(
                jnp.concatenate(
                    [
                        (first * scores_t[:half, :half]).astype(bf16),
                        (right * scores_t[:half, half:]).astype(bf16),
                    ],
                    axis=1,
                ),
                dmixed_b,
            )
            bottom = mm((last * scores_t[half:, half:]).astype(bf16), dmixed_b[half:])
            part = jnp.concatenate([top, bottom], axis=0)
            dscaled = part if dscaled is None else jnp.where(lane >= k * size, part, dscaled)
            dscores[:half, :half] += mm_nt(own[:half], dmixed_b[:half]) * first
            dscores[:half, half:] += mm_nt(own[:half], dmixed_b[half:]) * right
            dscores[half:, half:] += mm_nt(own[half:], dmixed_b[half:]) * last
        in_wide = mm_split(decay_in, spread)
        out_wide = mm_split(decay_out, spread)
        dheld = dstate[:, cols]
        dheld_b = dheld.astype(bf16)
        dstate_b[:, cols] = dheld_b
        dlate = out_wide * mm(keys, dheld_b)
        dscaled = dscaled + dlate
        rounded = scaled_b.astype(f32)
        dcumul = dcumul + mm_split(dmixed_b.astype(f32) * scanned - rounded * dscaled, gather)
        dsteps = dsteps + mm_split(inner * dscaled, gather)
        final_wide = in_wide[count - 1 : count, :]
        finals[0:1, cols] = jnp.sum(rounded * dlate, axis=0, keepdims=True) + final_wide * jnp.sum(
            dheld * states_ref[0, :, cols], axis=0, keepdims=True
        )
        dinner = dscaled * steps_wide + skip_ref[:, cols] * dmixed
        ext[0:count, cols] = dinner * (sig * (1.0 + conv * (1.0 - sig)))
        in_b = (in_wide * dmixed).astype(bf16)
        in_rows[:, cols] = in_b
        out_rows[:, cols] = (out_wide * scaled).astype(bf16)
        dstate[:, cols] = final_wide * dheld + mm(queries_t, in_b)

    pairs = dscores[...]
    dkeys = mm(pairs.astype(bf16), queries) + mm_nt(out_rows[...], dstate_b[...])
    dqueries = mm(pairs.T.astype(bf16), keys) + mm_nt(in_rows[...], states_ref[0].astype(bf16))
    ext[0:count, key_cols] = dkeys * (key_sig * (1.0 + key_pre * (1.0 - key_sig)))
    ext[0:count, query_cols] = dqueries * (query_sig * (1.0 + query_pre * (1.0 - query_sig)))

    for start in range(0, conv_width, LANES):
        cols = slice(start, start + LANES)
        pre = pre_ref[:, width + start : width + start + LANES]
        total = None
        for j in range(taps):
            moved = ext[taps - 1 - j : taps - 1 - j + count, cols]
            term = taps_ref[j : j + 1, cols] * moved
            total = term if total is None else total + term
            taps_grad_ref[j : j + 1, cols] += jnp.sum(pre * moved, axis=0, keepdims=True)
        taps_grad_ref[taps : taps + 1, cols] += jnp.sum(ext[0:count, cols], axis=0, keepdims=True)
        dpre_ref[:, width + start : width + start + LANES] = total.astype(bf16)
        ext[count : count + CARRY, cols] = ext[0:CARRY, cols]

    final_row = mm_split(jnp.broadcast_to(finals[0:1, :], (CARRY, width)), gather_ref[...])[0:1]
    suffix = 1.0 - tri_lower(count).astype(f32) + jnp.where(
        lax.broadcasted_iota(jnp.int32, (count, count), 0)
        == lax.broadcasted_iota(jnp.int32, (count, count), 1),
        1.0,
        0.0,
    )
    dlogs = mm_exact(suffix, dcumul) + final_row
    dshifted = (dsteps + dlogs * heads_ref[0:1, :]) * sigmoid(shifted)
    dpre_ref[:, width + conv_width :] = dshifted.astype(bf16)
    heads_grad_ref[0:1, :] += jnp.sum(dlogs * logs, axis=0, keepdims=True)
    heads_grad_ref[1:2, :] += jnp.sum(dshifted, axis=0, keepdims=True)


def whole(shape):
    return pl.BlockSpec(shape, lambda s, i: (0,) * len(shape))


def run_forward(pre, taps, heads, skip, spread, seqs, count, size):
    rows, cat = pre.shape
    width = skip.shape[1]
    conv_width = taps.shape[1]
    state_size = (conv_width - width) // 2
    blocks = rows // seqs // count

    def block(cols):
        return pl.BlockSpec((count, cols), lambda s, i: (s * blocks + i, 0))

    return pl.pallas_call(
        functools.partial(forward_kernel, width, size),
        grid=(seqs, blocks),
        in_specs=[block(cat), whole(taps.shape), whole(heads.shape), whole(skip.shape), whole(spread.shape)],
        out_specs=[
            block(width), block(conv_width), block(width), block(1),
            pl.BlockSpec((1, state_size, width), lambda s, i: (s * blocks + i, 0, 0)),
        ],
        out_shape=[
            jax.ShapeDtypeStruct((rows, width), f32),
            jax.ShapeDtypeStruct((rows, conv_width), f32),
            jax.ShapeDtypeStruct((rows, width), f32),
            jax.ShapeDtypeStruct((rows, 1), f32),
            jax.ShapeDtypeStruct((seqs * blocks, state_size, width), f32),
        ],
        scratch_shapes=[
            pltpu.VMEM((count + CARRY, conv_width), f32),
            pltpu.VMEM((state_size, width), f32),
            pltpu.VMEM((count, conv_width), f32),
        ],
        cost_estimate=pl.CostEstimate(
            flops=rows * width * count * 4, bytes_accessed=rows * (cat + 4 * width) * 4, transcendentals=rows * count * 12
        ),
        name="mixer_forward",
    )(pre, taps, heads, skip, spread)


def run_backward(pre, conv, scanned, dnormed, token, states, taps, heads, skip, gain, spread, gather, seqs, count, size):
    rows, cat = pre.shape
    width = skip.shape[1]
    conv_width = taps.shape[1]
    state_size = (conv_width - width) // 2
    blocks = rows // seqs // count

    def block(cols):
        return pl.BlockSpec((count, cols), lambda s, i: (s * blocks + blocks - 1 - i, 0))

    return pl.pallas_call(
        functools.partial(backward_kernel, width, size),
        grid=(seqs, blocks),
        in_specs=[
            block(cat), block(conv_width), block(width), block(width), block(2),
            pl.BlockSpec((1, state_size, width), lambda s, i: (s * blocks + blocks - 1 - i, 0, 0)),
            whole(taps.shape), whole(heads.shape), whole(skip.shape), whole(gain.shape),
            whole(spread.shape), whole(gather.shape),
        ],
        out_specs=[block(cat), whole((8, conv_width)), whole((8, width)), whole((8, LANES))],
        out_shape=[
            jax.ShapeDtypeStruct((rows, cat), bf16),
            jax.ShapeDtypeStruct((8, conv_width), f32),
            jax.ShapeDtypeStruct((8, width), f32),
            jax.ShapeDtypeStruct((8, LANES), f32),
        ],
        scratch_shapes=[
            pltpu.VMEM((count + CARRY, conv_width), f32),
            pltpu.VMEM((state_size, width), f32),
            pltpu.VMEM((count, count), f32),
            pltpu.VMEM((count, width), bf16),
            pltpu.VMEM((count, width), bf16),
            pltpu.VMEM((state_size, width), bf16),
            pltpu.VMEM((8, width), f32),
        ],
        cost_estimate=pl.CostEstimate(
            flops=rows * width * count * 8, bytes_accessed=rows * (2 * cat + 4 * width) * 4, transcendentals=rows * count * 12
        ),
        name="mixer_backward",
    )(pre, conv, scanned, dnormed, token, states, taps, heads, skip, gain, spread, gather)


def adam_step(param, first, second_moment, grad, rate):
    first_new = beta_first * first + (1.0 - beta_first) * grad
    second_new = beta_second * second_moment + (1.0 - beta_second) * grad * grad
    first_hat = first_new / (1.0 - beta_first**step_count)
    second_hat = second_new / (1.0 - beta_second**step_count)
    moved = param - rate * (first_hat / (jnp.sqrt(second_hat) + adam_eps) + decay_rate * param)
    return (moved, first_new, second_new)


def body(hidden, cotangent, *arrays):
    params, firsts, seconds = arrays[:9], arrays[9:18], arrays[18:27]
    (
        input_gain,
        inner_weight,
        step_weight,
        state_weight,
        inner_taps,
        state_taps,
        head_params,
        gated_gain,
        output_matrix,
    ) = params
    local_len, seqs, features = hidden.shape
    wide = inner_taps.shape[1]
    heads = head_params.shape[1]
    size = wide // heads
    states = state_taps.shape[1]
    shards = lax.axis_size("tensor")
    length = local_len * shards
    rows = length * seqs
    inner_total = wide * shards

    base = hidden.astype(f32)
    rstd = lax.rsqrt(jnp.mean(base * base, -1, keepdims=True) + norm_eps)
    normed = base * rstd
    normed_in = (normed * input_gain).astype(bf16)

    def by_sequence(values):
        return values.transpose(1, 0, 2).reshape(values.shape[0] * seqs, values.shape[2])

    def by_position(values):
        return values.reshape(seqs, values.shape[0] // seqs, values.shape[1]).transpose(1, 0, 2)

    state_rows = lax.all_gather(state_weight.astype(bf16), "tensor", axis=0, tiled=True)
    full_in = lax.all_gather(normed_in, "tensor", axis=0, tiled=True)
    weights_own = jnp.concatenate(
        [
            inner_weight[0].astype(bf16),
            inner_weight[1].astype(bf16),
            state_rows,
            jnp.pad(step_weight.astype(bf16), ((0, 0), (0, LANES - heads))),
        ],
        axis=1,
    )
    weights = lax.all_gather(weights_own, "dp", axis=0, tiled=True)
    output_t = lax.all_gather(output_matrix.astype(bf16).T, "dp", axis=0, tiled=True)
    full_cot = lax.all_gather(cotangent, "tensor", axis=0, tiled=True)
    flat_in = by_sequence(full_in)
    flat_cot = by_sequence(full_cot)

    taps = jnp.concatenate([inner_taps, state_taps], axis=1)
    head_rows = jnp.pad(
        jnp.stack([-jnp.exp(head_params[0]), head_params[1]]), ((0, 0), (0, LANES - heads))
    )
    skip = jnp.repeat(head_params[2], size)[None]
    gain = gated_gain[None]
    spread = (jnp.arange(LANES)[:, None] == jnp.arange(wide)[None] // size).astype(bf16)
    gather = (jnp.arange(wide)[:, None] // size == jnp.arange(LANES)[None]).astype(bf16)

    pre = mm(flat_in, weights)
    scanned, conv, gated, squares, chunk_states = run_forward(
        pre, taps, head_rows, skip, spread, seqs, GROUP, size
    )
    d_normed = mm(flat_cot, output_t)
    crossed = jnp.sum(d_normed * gain * gated, -1, keepdims=True)
    sums = lax.psum(jnp.concatenate([squares, crossed], axis=1), "tensor")
    scale = lax.rsqrt(sums[:, 0:1] / inner_total + norm_eps)
    token = jnp.concatenate(
        [scale, scale * scale * scale * (sums[:, 1:2] / inner_total)], axis=1
    )
    normed_out = (gated * scale * gain).astype(bf16)
    branch = lax.psum_scatter(
        by_position(mm_nt(normed_out, output_t)).astype(bf16),
        "tensor",
        scatter_dimension=0,
        tiled=True,
    )
    result = (base + branch.astype(f32)).astype(bf16)
    grad_output_t = lax.psum_scatter(
        contract_first(flat_cot, normed_out).astype(bf16), "dp", scatter_dimension=0, tiled=True
    )

    d_pre, taps_grad, wide_grad, head_grad = run_backward(
        pre, conv, scanned, d_normed, token, chunk_states, taps, head_rows, skip, gain,
        spread, gather, seqs, GROUP, size,
    )
    d_in = lax.psum_scatter(
        by_position(mm_nt(d_pre, weights)).astype(bf16),
        "tensor",
        scatter_dimension=0,
        tiled=True,
    ).astype(f32)
    grad_weights = contract_first(flat_in, d_pre)
    grad_own = lax.psum_scatter(
        grad_weights.astype(bf16), "dp", scatter_dimension=0, tiled=True
    )
    grad_gain_rows = jnp.sum(grad_weights * weights.astype(f32), axis=1) / input_gain
    grad_state = lax.psum_scatter(
        grad_own[:, 2 * wide : 2 * wide + states].astype(f32),
        "tensor",
        scatter_dimension=0,
        tiled=True,
    )

    d_hat = d_in * input_gain
    gradient_hidden = cotangent.astype(f32) + rstd * (
        d_hat - normed * jnp.mean(d_hat * normed, -1, keepdims=True)
    )
    grad_skip = jnp.sum(wide_grad[1].reshape(heads, size), axis=1)
    split_terms = (
        taps_grad[: inner_taps.shape[0], :wide],
        jnp.concatenate([head_grad[:2, :heads], grad_skip[None]], axis=0),
        wide_grad[0],
    )
    shared_terms = (grad_gain_rows, taps_grad[: state_taps.shape[0], wide:])
    split_sums = lax.psum(split_terms, "dp")
    shared_sums = lax.psum(shared_terms, ("dp", "tensor"))
    own = grad_own.astype(f32)
    grads = (
        shared_sums[0],
        jnp.stack([own[:, :wide], own[:, wide : 2 * wide]]),
        own[:, 2 * wide + states : 2 * wide + states + heads],
        grad_state,
        split_sums[0],
        shared_sums[1],
        split_sums[1],
        split_sums[2],
        grad_output_t.astype(f32).T,
    )
    stepped = [
        adam_step(param, first, second_moment, grad, rate)
        for param, first, second_moment, grad, rate in zip(params, firsts, seconds, grads, rates)
    ]
    moved = [entry[0] for entry in stepped]
    first_new = [entry[1] for entry in stepped]
    second_new = [entry[2] for entry in stepped]
    return (result, gradient_hidden, *grads, *moved, *first_new, *second_new)


def contract_first(left, right):
    return lax.dot_general(left, right, (((0,), (0,)), ((), ())), preferred_element_type=f32)


def solution(mesh):
    weights = (
        P(),
        P(None, "dp", "tensor"),
        P("dp", "tensor"),
        P(("dp", "tensor"), None),
        P(None, "tensor"),
        P(),
        P(None, "tensor"),
        P("tensor"),
        P("tensor", "dp"),
    )
    rows = P("tensor", "dp", None)
    return jax.shard_map(
        body,
        mesh=mesh,
        in_specs=(rows, rows) + weights * 3,
        out_specs=(rows, rows) + weights * 4,
        check_vma=False,
    )
```

```python
import functools
import jax
import jax.numpy as jnp
from jax import lax
from jax.experimental import pallas as pl
from jax.experimental.pallas import tpu as pltpu
from jax.sharding import PartitionSpec as P

GROUP = 256
norm_eps = 1e-05
beta_first = 0.9
beta_second = 0.95
adam_eps = 1e-08
decay_rate = 0.1
step_count = 4.0
rates = (0.2, 0.008, 0.008, 0.008, 0.1, 0.1, 0.4, 0.2, 0.006)

LANES = 128
CARRY = 8
BLOCKED = -1e30
f32 = jnp.float32
bf16 = jnp.bfloat16


def mm(a, b):
    return lax.dot_general(a, b, (((1,), (0,)), ((), ())), preferred_element_type=f32)


def mm_nt(a, b):
    return lax.dot_general(a, b, (((1,), (1,)), ((), ())), preferred_element_type=f32)


def mm_exact(a, b):
    return lax.dot_general(
        a, b, (((1,), (0,)), ((), ())), precision=lax.Precision.HIGHEST, preferred_element_type=f32
    )


def mm_split(values, weight):
    high = values.astype(bf16)
    low = (values - high.astype(f32)).astype(bf16)
    return mm(high, weight) + mm(low, weight)


MESH = pl.DeviceIdType.MESH


def meet(peers, beside=()):
    barrier = pltpu.get_barrier_semaphore()
    for peer in peers:
        pl.semaphore_signal(barrier, inc=1, device_id={"dp": peer}, device_id_type=MESH)
    for peer in beside:
        pl.semaphore_signal(barrier, inc=1, device_id={"tensor": peer}, device_id_type=MESH)
    pl.semaphore_wait(barrier, len(peers) + len(beside))


def send(source, target, send_sem, recv_sem, peer, axis="dp"):
    return pltpu.make_async_remote_copy(
        src_ref=source,
        dst_ref=target,
        send_sem=send_sem,
        recv_sem=recv_sem,
        device_id={axis: peer},
        device_id_type=MESH,
    )


def gather_kernel(n, own_ref, full_ref, own_sem, far_send, far_recv, near_send, near_recv):
    rows = own_ref.shape[0]
    chips = n // 2
    me = lax.axis_index("dp")
    core = lax.rem(me, 2)
    chip = me // 2
    partner = me + 1 - 2 * core
    others = [2 * lax.rem(chip + 1 + k, chips) + core for k in range(chips - 1)]
    meet(others + [partner])

    def place(index):
        return full_ref.at[pl.ds(pl.multiple_of(index * rows, rows), rows), :]

    far = [
        send(own_ref, place(me), far_send.at[k], far_recv.at[k], others[k]) for k in range(chips - 1)
    ]
    for copy in far:
        copy.start()
    near = [send(own_ref, place(me), near_send.at[chips - 1], near_recv.at[chips - 1], partner)]
    near[0].start()
    kept = pltpu.make_async_copy(own_ref, place(me), own_sem)
    kept.start()
    for k in range(chips - 1):
        source = 2 * lax.rem(chip + chips - 1 - k, chips) + core
        far[k].wait_recv()
        copy = send(place(source), place(source), near_send.at[k], near_recv.at[k], partner)
        copy.start()
        near.append(copy)
    kept.wait()
    for copy in far:
        copy.wait_send()
    for copy in near:
        copy.wait()


def gather_dp(own, n):
    rows, cols = own.shape
    return pl.pallas_call(
        functools.partial(gather_kernel, n),
        out_shape=jax.ShapeDtypeStruct((rows * n, cols), own.dtype),
        in_specs=[pl.BlockSpec(memory_space=pltpu.VMEM)],
        out_specs=pl.BlockSpec(memory_space=pl.ANY),
        scratch_shapes=[
            pltpu.SemaphoreType.DMA(()),
            pltpu.SemaphoreType.DMA((n // 2 - 1,)),
            pltpu.SemaphoreType.DMA((n // 2 - 1,)),
            pltpu.SemaphoreType.DMA((n // 2,)),
            pltpu.SemaphoreType.DMA((n // 2,)),
        ],
        compiler_params=pltpu.CompilerParams(collective_id=0, has_side_effects=True),
        cost_estimate=pl.CostEstimate(flops=0, bytes_accessed=240_000_000, transcendentals=0),
        name="gather_dp",
    )(own)


class Exchange:
    def __init__(self, n, terms, near_buf, out_buf, far_buf, near_send, near_recv, far_send, far_recv):
        self.n, self.terms, self.near_buf, self.out_buf, self.far_buf = n, terms, near_buf, out_buf, far_buf
        self.near_send, self.near_recv, self.far_send, self.far_recv = near_send, near_recv, far_send, far_recv
        self.chips = n // 2
        self.rows = terms.shape[0] // n
        me = lax.axis_index("dp")
        self.core = lax.rem(me, 2)
        self.partner = me + 1 - 2 * self.core
        self.order = [lax.rem(me // 2 + 1 + k, self.chips) for k in range(self.chips)]

    def block(self, index):
        return pl.ds(pl.multiple_of(index * self.rows, self.rows), self.rows)

    def near(self, k):
        index = 2 * self.order[k] + 1 - self.core
        return send(
            self.terms.at[self.block(index), :], self.near_buf.at[k],
            self.near_send.at[k], self.near_recv.at[k], self.partner,
        )

    def far(self, k):
        return send(
            self.out_buf.at[k], self.far_buf.at[k],
            self.far_send.at[k], self.far_recv.at[k], 2 * self.order[k] + self.core,
        )

    def start(self):
        for k in range(self.chips):
            self.near(k).start()

    def pair_sum(self, k):
        return self.terms[self.block(2 * self.order[k] + self.core), :] + self.near_buf[k]

    def forward(self):
        for k in range(self.chips - 1):
            self.near(k).wait()
            self.out_buf[k] = self.pair_sum(k).astype(bf16)
            self.far(k).start()

    def finish(self):
        self.near(self.chips - 1).wait()
        total = self.pair_sum(self.chips - 1)
        for k in range(self.chips - 1):
            self.far(k).wait()
            total = total + self.far_buf[k].astype(f32)
        return total

    @staticmethod
    def scratch(n, rows, cols):
        chips = n // 2
        return [
            pltpu.VMEM((chips, rows, cols), f32),
            pltpu.VMEM((chips - 1, rows, cols), bf16),
            pltpu.VMEM((chips - 1, rows, cols), bf16),
            pltpu.SemaphoreType.DMA((chips,)),
            pltpu.SemaphoreType.DMA((chips,)),
            pltpu.SemaphoreType.DMA((chips - 1,)),
            pltpu.SemaphoreType.DMA((chips - 1,)),
        ]


def all_others(n, axis="dp"):
    me = lax.axis_index(axis)
    return [lax.rem(me + 1 + k, n) for k in range(n - 1)]


def sum_kernel(
    n, shards, start, terms_ref, small_ref, own_ref, small_out_ref, shared_ref, state_ref, *scratch
):
    small_buf, small_send, small_recv, state_out, state_buf, shared_buf = scratch[7:13]
    state_send, state_recv, shared_send, shared_recv = scratch[13:]
    others = all_others(n)
    beside = all_others(shards, "tensor")
    meet(others, beside)
    exchange = Exchange(n, terms_ref, *scratch[:7])
    exchange.start()
    copies = [
        send(small_ref, small_buf.at[k], small_send.at[k], small_recv.at[k], others[k])
        for k in range(n - 1)
    ]
    for copy in copies:
        copy.start()
    exchange.forward()
    small = small_ref[...]
    for k in range(n - 1):
        copies[k].wait()
        small = small + small_buf[k]
    small_out_ref[...] = small
    own_ref[...] = exchange.finish()
    rows, cols = state_ref.shape
    for k in range(shards):
        state_out[k] = own_ref[k * rows : (k + 1) * rows, start : start + cols]
    shared = [
        send(small_out_ref, shared_buf.at[k], shared_send.at[k], shared_recv.at[k], beside[k], "tensor")
        for k in range(shards - 1)
    ]
    parts = [
        send(
            state_out.at[beside[k]], state_buf.at[k], state_send.at[k], state_recv.at[k], beside[k], "tensor"
        )
        for k in range(shards - 1)
    ]
    for copy in shared + parts:
        copy.start()
    total = state_out[lax.axis_index("tensor")]
    for k in range(shards - 1):
        shared[k].wait()
        small = small + shared_buf[k]
    shared_ref[...] = small
    for k in range(shards - 1):
        parts[k].wait()
        total = total + state_buf[k]
    state_ref[...] = total


def sum_dp(terms, small, n, shards, start, states):
    rows, cols = terms.shape[0] // n, terms.shape[1]
    part = (rows // shards, states)
    vmem = pl.BlockSpec(memory_space=pltpu.VMEM)
    return pl.pallas_call(
        functools.partial(sum_kernel, n, shards, start),
        out_shape=[
            jax.ShapeDtypeStruct((rows, cols), f32),
            jax.ShapeDtypeStruct(small.shape, f32),
            jax.ShapeDtypeStruct(small.shape, f32),
            jax.ShapeDtypeStruct(part, f32),
        ],
        in_specs=[vmem, vmem],
        out_specs=[vmem, vmem, vmem, vmem],
        scratch_shapes=Exchange.scratch(n, rows, cols)
        + [
            pltpu.VMEM((n - 1,) + small.shape, f32),
            pltpu.SemaphoreType.DMA((n - 1,)),
            pltpu.SemaphoreType.DMA((n - 1,)),
            pltpu.VMEM((shards,) + part, f32),
            pltpu.VMEM((shards - 1,) + part, f32),
            pltpu.VMEM((shards - 1,) + small.shape, f32),
        ]
        + [pltpu.SemaphoreType.DMA((shards - 1,))] * 4,
        compiler_params=pltpu.CompilerParams(
            collective_id=1, has_side_effects=True, vmem_limit_bytes=56 * 1024 * 1024
        ),
        cost_estimate=pl.CostEstimate(flops=0, bytes_accessed=240_000_000, transcendentals=0),
        name="sum_dp",
    )(terms, small)


def token_kernel(shards, own_ref, total_ref, buf, send_sem, recv_sem):
    beside = all_others(shards, "tensor")
    meet((), beside)
    copies = [
        send(own_ref, buf.at[k], send_sem.at[k], recv_sem.at[k], beside[k], "tensor")
        for k in range(shards - 1)
    ]
    for copy in copies:
        copy.start()
    total = own_ref[...]
    for k in range(shards - 1):
        copies[k].wait()
        total = total + buf[k]
    total_ref[...] = total


def sum_tensor(own, shards):
    vmem = pl.BlockSpec(memory_space=pltpu.VMEM)
    return pl.pallas_call(
        functools.partial(token_kernel, shards),
        out_shape=jax.ShapeDtypeStruct(own.shape, f32),
        in_specs=[vmem],
        out_specs=vmem,
        scratch_shapes=[
            pltpu.VMEM((shards - 1,) + own.shape, f32),
            pltpu.SemaphoreType.DMA((shards - 1,)),
            pltpu.SemaphoreType.DMA((shards - 1,)),
        ],
        compiler_params=pltpu.CompilerParams(collective_id=3, has_side_effects=True),
        name="sum_tensor",
    )(own)


def sigmoid(v):
    return 1.0 / (1.0 + jnp.exp(-v))


def tri_lower(count):
    rows = lax.broadcasted_iota(jnp.int32, (count, count), 0)
    cols = lax.broadcasted_iota(jnp.int32, (count, count), 1)
    return rows >= cols


def step_terms(step_pre, heads_ref):
    shifted = step_pre + heads_ref[1:2, :]
    steps = jnp.maximum(shifted, 0.0) + jnp.log1p(jnp.exp(-jnp.abs(shifted)))
    logs = heads_ref[0:1, :] * steps
    count = logs.shape[0]
    cumul = mm_exact(tri_lower(count).astype(f32), logs)
    return shifted, steps, logs, cumul


def forward_kernel(
    width, size, pre_ref, taps_ref, heads_ref, skip_ref, spread_ref,
    scanned_ref, conv_ref, gated_ref, states_ref,
    ext, state, act,
):
    count = pre_ref.shape[0]
    half = count // 2
    conv_width = taps_ref.shape[1]
    taps = taps_ref.shape[0] - 1
    state_size = (conv_width - width) // 2
    per_tile = LANES // size

    @pl.when(pl.program_id(1) == 0)
    def _():
        ext[0:CARRY, :] = jnp.zeros((CARRY, conv_width), f32)
        state[...] = jnp.zeros_like(state)

    states_ref[0] = state[...]
    for start in range(0, conv_width, LANES):
        cols = slice(start, start + LANES)
        ext[CARRY : CARRY + count, cols] = pre_ref[:, width + start : width + start + LANES]
        total = taps_ref[taps : taps + 1, cols]
        for j in range(taps):
            total = total + taps_ref[j : j + 1, cols] * ext[CARRY + 1 - taps + j : CARRY + 1 - taps + j + count, cols]
        conv_ref[:, cols] = total
        act[:, cols] = total * sigmoid(total)
        ext[0:CARRY, cols] = ext[count : count + CARRY, cols]

    _, steps, _, cumul = step_terms(pre_ref[:, width + conv_width :], heads_ref)
    cumul_t = cumul.T
    final = cumul[count - 1 : count, :]
    decay_in = jnp.exp(cumul)
    decay_out = jnp.exp(final - cumul)
    keys = act[:, width : width + state_size].astype(bf16)
    queries = act[:, width + state_size :].astype(bf16)
    keys_t = act[:, width : width + state_size].T.astype(bf16)
    scores = mm_nt(queries, keys)
    causal = tri_lower(half)
    lane = lax.broadcasted_iota(jnp.int32, (count, LANES), 1)
    for tile in range(width // LANES):
        cols = slice(tile * LANES, (tile + 1) * LANES)
        spread = spread_ref[:, cols]
        inner = act[:, cols]
        scaled = inner * mm_split(steps, spread)
        scaled_b = scaled.astype(bf16)
        mixed = None
        for k in range(per_tile):
            head = tile * per_tile + k
            col = cumul[:, head : head + 1]
            row = cumul_t[head : head + 1, :]
            first = jnp.exp(jnp.where(causal, col[:half] - row[:, :half], BLOCKED)) * scores[:half, :half]
            low = jnp.exp(col[half:] - row[:, :half]) * scores[half:, :half]
            last = jnp.exp(jnp.where(causal, col[half:] - row[:, half:], BLOCKED)) * scores[half:, half:]
            top = mm(first.astype(bf16), scaled_b[:half])
            bottom = mm(jnp.concatenate([low.astype(bf16), last.astype(bf16)], axis=1), scaled_b)
            part = jnp.concatenate([top, bottom], axis=0)
            mixed = part if mixed is None else jnp.where(lane >= k * size, part, mixed)
        in_wide = mm_split(decay_in, spread)
        out_wide = mm_split(decay_out, spread)
        held = state[:, cols]
        scanned = mixed + in_wide * mm(queries, held.astype(bf16))
        state[:, cols] = in_wide[count - 1 : count, :] * held + mm(keys_t, (out_wide * scaled).astype(bf16))
        scanned_ref[:, cols] = scanned
        gate = pre_ref[:, cols]
        gated = (scanned + skip_ref[:, cols] * inner) * (gate * sigmoid(gate))
        gated_ref[:, cols] = gated


def backward_kernel(
    n, width, size, pre_ref, conv_ref, scanned_ref, dnormed_ref, token_ref, states_ref,
    taps_ref, heads_ref, skip_ref, gain_ref, spread_ref, gather_ref, terms_ref,
    dpre_ref, taps_grad_ref, wide_grad_ref, heads_grad_ref, own_ref,
    ext, dstate, dscores, in_rows, out_rows, dstate_b, finals, *scratch,
):
    exchange = Exchange(n, terms_ref, *scratch)
    opening = (pl.program_id(0) == 0) & (pl.program_id(1) == 0)
    middle = (pl.program_id(0) == 0) & (pl.program_id(1) == 1)
    closing = (pl.program_id(0) == pl.num_programs(0) - 1) & (pl.program_id(1) == pl.num_programs(1) - 1)

    @pl.when(opening)
    def _():
        meet(all_others(n))
        exchange.start()

    @pl.when(middle)
    def _():
        exchange.forward()

    count = pre_ref.shape[0]
    half = count // 2
    conv_width = taps_ref.shape[1]
    taps = taps_ref.shape[0] - 1
    state_size = (conv_width - width) // 2
    per_tile = LANES // size

    @pl.when(pl.program_id(1) == 0)
    def _():
        ext[count : count + CARRY, :] = jnp.zeros((CARRY, conv_width), f32)
        dstate[...] = jnp.zeros_like(dstate)

    @pl.when(opening)
    def _():
        taps_grad_ref[...] = jnp.zeros_like(taps_grad_ref)
        wide_grad_ref[...] = jnp.zeros_like(wide_grad_ref)
        heads_grad_ref[...] = jnp.zeros_like(heads_grad_ref)

    shifted, steps, logs, cumul = step_terms(pre_ref[:, width + conv_width :], heads_ref)
    cumul_t = cumul.T
    final = cumul[count - 1 : count, :]
    decay_in = jnp.exp(cumul)
    decay_out = jnp.exp(final - cumul)
    key_cols = slice(width, width + state_size)
    query_cols = slice(width + state_size, conv_width)
    key_pre = conv_ref[:, key_cols]
    query_pre = conv_ref[:, query_cols]
    key_sig = sigmoid(key_pre)
    query_sig = sigmoid(query_pre)
    keys = (key_pre * key_sig).astype(bf16)
    queries = (query_pre * query_sig).astype(bf16)
    queries_t = (query_pre * query_sig).T.astype(bf16)
    scores_t = mm_nt(keys, queries)
    rows = lax.broadcasted_iota(jnp.int32, (half, half), 0)
    columns = lax.broadcasted_iota(jnp.int32, (half, half), 1)
    causal_t = columns >= rows
    lane = lax.broadcasted_iota(jnp.int32, (count, LANES), 1)
    dscores[...] = jnp.zeros_like(dscores)
    scale = token_ref[:, 0:1]
    pull = token_ref[:, 1:2]
    dcumul = jnp.zeros((count, LANES), f32)
    dsteps = jnp.zeros((count, LANES), f32)
    for tile in range(width // LANES):
        cols = slice(tile * LANES, (tile + 1) * LANES)
        spread = spread_ref[:, cols]
        gather = gather_ref[cols, :]
        conv = conv_ref[:, cols]
        sig = sigmoid(conv)
        inner = conv * sig
        gate = pre_ref[:, cols]
        gate_sig = sigmoid(gate)
        gate_act = gate * gate_sig
        scanned = scanned_ref[:, cols]
        mixed = scanned + skip_ref[:, cols] * inner
        gated = mixed * gate_act
        dnormed = dnormed_ref[:, cols]
        wide_grad_ref[0:1, cols] += jnp.sum(dnormed * gated * scale, axis=0, keepdims=True)
        dgated = scale * (dnormed * gain_ref[:, cols]) - pull * gated
        dmixed = dgated * gate_act
        dgate = dgated * mixed * (gate_sig * (1.0 + gate * (1.0 - gate_sig)))
        dpre_ref[:, cols] = dgate.astype(bf16)
        wide_grad_ref[1:2, cols] += jnp.sum(dmixed * inner, axis=0, keepdims=True)
        dmixed_b = dmixed.astype(bf16)
        steps_wide = mm_split(steps, spread)
        scaled = inner * steps_wide
        scaled_b = scaled.astype(bf16)
        dscaled = None
        for k in range(per_tile):
            head = tile * per_tile + k
            col = cumul[:, head : head + 1]
            row = cumul_t[head : head + 1, :]
            own = jnp.where((lane >= k * size) & (lane < (k + 1) * size), scaled, 0.0).astype(bf16)
            first = jnp.exp(jnp.where(causal_t, row[:, :half] - col[:half], BLOCKED))
            right = jnp.exp(row[:, half:] - col[:half])
            last = jnp.exp(jnp.where(causal_t, row[:, half:] - col[half:], BLOCKED))
            top = mm(
                jnp.concatenate(
                    [
                        (first * scores_t[:half, :half]).astype(bf16),
                        (right * scores_t[:half, half:]).astype(bf16),
                    ],
                    axis=1,
                ),
                dmixed_b,
            )
            bottom = mm((last * scores_t[half:, half:]).astype(bf16), dmixed_b[half:])
            part = jnp.concatenate([top, bottom], axis=0)
            dscaled = part if dscaled is None else jnp.where(lane >= k * size, part, dscaled)
            dscores[:half, :half] += mm_nt(own[:half], dmixed_b[:half]) * first
            dscores[:half, half:] += mm_nt(own[:half], dmixed_b[half:]) * right
            dscores[half:, half:] += mm_nt(own[half:], dmixed_b[half:]) * last
        in_wide = mm_split(decay_in, spread)
        out_wide = mm_split(decay_out, spread)
        dheld = dstate[:, cols]
        dheld_b = dheld.astype(bf16)
        dstate_b[:, cols] = dheld_b
        dlate = out_wide * mm(keys, dheld_b)
        dscaled = dscaled + dlate
        rounded = scaled_b.astype(f32)
        dcumul = dcumul + mm_split(dmixed_b.astype(f32) * scanned - rounded * dscaled, gather)
        dsteps = dsteps + mm_split(inner * dscaled, gather)
        final_wide = in_wide[count - 1 : count, :]
        finals[0:1, cols] = jnp.sum(rounded * dlate, axis=0, keepdims=True) + final_wide * jnp.sum(
            dheld * states_ref[0, :, cols], axis=0, keepdims=True
        )
        dinner = dscaled * steps_wide + skip_ref[:, cols] * dmixed
        ext[0:count, cols] = dinner * (sig * (1.0 + conv * (1.0 - sig)))
        in_b = (in_wide * dmixed).astype(bf16)
        in_rows[:, cols] = in_b
        out_rows[:, cols] = (out_wide * scaled).astype(bf16)
        dstate[:, cols] = final_wide * dheld + mm(queries_t, in_b)

    pairs = dscores[...]
    dkeys = mm(pairs.astype(bf16), queries) + mm_nt(out_rows[...], dstate_b[...])
    dqueries = mm(pairs.T.astype(bf16), keys) + mm_nt(in_rows[...], states_ref[0].astype(bf16))
    ext[0:count, key_cols] = dkeys * (key_sig * (1.0 + key_pre * (1.0 - key_sig)))
    ext[0:count, query_cols] = dqueries * (query_sig * (1.0 + query_pre * (1.0 - query_sig)))

    for start in range(0, conv_width, LANES):
        cols = slice(start, start + LANES)
        pre = pre_ref[:, width + start : width + start + LANES]
        total = None
        for j in range(taps):
            moved = ext[taps - 1 - j : taps - 1 - j + count, cols]
            term = taps_ref[j : j + 1, cols] * moved
            total = term if total is None else total + term
            taps_grad_ref[j : j + 1, cols] += jnp.sum(pre * moved, axis=0, keepdims=True)
        taps_grad_ref[taps : taps + 1, cols] += jnp.sum(ext[0:count, cols], axis=0, keepdims=True)
        dpre_ref[:, width + start : width + start + LANES] = total.astype(bf16)
        ext[count : count + CARRY, cols] = ext[0:CARRY, cols]

    final_row = mm_split(jnp.broadcast_to(finals[0:1, :], (CARRY, width)), gather_ref[...])[0:1]
    suffix = 1.0 - tri_lower(count).astype(f32) + jnp.where(
        lax.broadcasted_iota(jnp.int32, (count, count), 0)
        == lax.broadcasted_iota(jnp.int32, (count, count), 1),
        1.0,
        0.0,
    )
    dlogs = mm_exact(suffix, dcumul) + final_row
    dshifted = (dsteps + dlogs * heads_ref[0:1, :]) * sigmoid(shifted)
    dpre_ref[:, width + conv_width :] = dshifted.astype(bf16)
    heads_grad_ref[0:1, :] += jnp.sum(dlogs * logs, axis=0, keepdims=True)
    heads_grad_ref[1:2, :] += jnp.sum(dshifted, axis=0, keepdims=True)

    @pl.when(closing)
    def _():
        own_ref[...] = exchange.finish()


def whole(shape):
    return pl.BlockSpec(shape, lambda s, i: (0,) * len(shape))


def run_forward(pre, taps, heads, skip, spread, seqs, count, size):
    rows, cat = pre.shape
    width = skip.shape[1]
    conv_width = taps.shape[1]
    state_size = (conv_width - width) // 2
    blocks = rows // seqs // count

    def block(cols):
        return pl.BlockSpec((count, cols), lambda s, i: (s * blocks + i, 0))

    return pl.pallas_call(
        functools.partial(forward_kernel, width, size),
        grid=(seqs, blocks),
        in_specs=[block(cat), whole(taps.shape), whole(heads.shape), whole(skip.shape), whole(spread.shape)],
        out_specs=[
            block(width), block(conv_width), block(width),
            pl.BlockSpec((1, state_size, width), lambda s, i: (s * blocks + i, 0, 0)),
        ],
        out_shape=[
            jax.ShapeDtypeStruct((rows, width), f32),
            jax.ShapeDtypeStruct((rows, conv_width), f32),
            jax.ShapeDtypeStruct((rows, width), f32),
            jax.ShapeDtypeStruct((seqs * blocks, state_size, width), f32),
        ],
        scratch_shapes=[
            pltpu.VMEM((count + CARRY, conv_width), f32),
            pltpu.VMEM((state_size, width), f32),
            pltpu.VMEM((count, conv_width), f32),
        ],
        cost_estimate=pl.CostEstimate(
            flops=rows * width * count * 4, bytes_accessed=rows * (cat + 4 * width) * 4, transcendentals=rows * count * 12
        ),
        name="mixer_forward",
    )(pre, taps, heads, skip, spread)


def run_backward(pre, conv, scanned, dnormed, token, states, taps, heads, skip, gain, spread, gather, terms, n, seqs, count, size):
    rows, cat = pre.shape
    width = skip.shape[1]
    conv_width = taps.shape[1]
    state_size = (conv_width - width) // 2
    blocks = rows // seqs // count

    def block(cols):
        return pl.BlockSpec((count, cols), lambda s, i: (s * blocks + blocks - 1 - i, 0))

    return pl.pallas_call(
        functools.partial(backward_kernel, n, width, size),
        grid=(seqs, blocks),
        in_specs=[
            block(cat), block(conv_width), block(width), block(width), block(2),
            pl.BlockSpec((1, state_size, width), lambda s, i: (s * blocks + blocks - 1 - i, 0, 0)),
            whole(taps.shape), whole(heads.shape), whole(skip.shape), whole(gain.shape),
            whole(spread.shape), whole(gather.shape),
            pl.BlockSpec(memory_space=pltpu.VMEM),
        ],
        out_specs=[
            block(cat), whole((8, conv_width)), whole((8, width)), whole((8, LANES)),
            whole((terms.shape[0] // n, terms.shape[1])),
        ],
        out_shape=[
            jax.ShapeDtypeStruct((rows, cat), bf16),
            jax.ShapeDtypeStruct((8, conv_width), f32),
            jax.ShapeDtypeStruct((8, width), f32),
            jax.ShapeDtypeStruct((8, LANES), f32),
            jax.ShapeDtypeStruct((terms.shape[0] // n, terms.shape[1]), f32),
        ],
        scratch_shapes=[
            pltpu.VMEM((count + CARRY, conv_width), f32),
            pltpu.VMEM((state_size, width), f32),
            pltpu.VMEM((count, count), f32),
            pltpu.VMEM((count, width), bf16),
            pltpu.VMEM((count, width), bf16),
            pltpu.VMEM((state_size, width), bf16),
            pltpu.VMEM((8, width), f32),
        ]
        + Exchange.scratch(n, terms.shape[0] // n, terms.shape[1]),
        compiler_params=pltpu.CompilerParams(
            collective_id=2, has_side_effects=True, vmem_limit_bytes=56 * 1024 * 1024
        ),
        cost_estimate=pl.CostEstimate(
            flops=rows * width * count * 8, bytes_accessed=rows * (2 * cat + 4 * width) * 4, transcendentals=rows * count * 12
        ),
        name="mixer_backward",
    )(pre, conv, scanned, dnormed, token, states, taps, heads, skip, gain, spread, gather, terms)


def adam_step(param, first, second_moment, grad, rate):
    first_new = beta_first * first + (1.0 - beta_first) * grad
    second_new = beta_second * second_moment + (1.0 - beta_second) * grad * grad
    first_hat = first_new / (1.0 - beta_first**step_count)
    second_hat = second_new / (1.0 - beta_second**step_count)
    moved = param - rate * (first_hat / (jnp.sqrt(second_hat) + adam_eps) + decay_rate * param)
    return (moved, first_new, second_new)


def body(hidden, cotangent, *arrays):
    params, firsts, seconds = arrays[:9], arrays[9:18], arrays[18:27]
    (
        input_gain,
        inner_weight,
        step_weight,
        state_weight,
        inner_taps,
        state_taps,
        head_params,
        gated_gain,
        output_matrix,
    ) = params
    _, seqs, features = hidden.shape
    wide = inner_taps.shape[1]
    heads = head_params.shape[1]
    size = wide // heads
    states = state_taps.shape[1]
    shards = lax.axis_size("tensor")
    inner_total = wide * shards

    base = hidden.astype(f32)
    rstd = lax.rsqrt(jnp.mean(base * base, -1, keepdims=True) + norm_eps)
    normed = base * rstd
    normed_in = (normed * input_gain).astype(bf16)

    def by_sequence(values):
        return values.transpose(1, 0, 2).reshape(values.shape[0] * seqs, values.shape[2])

    def by_position(values):
        return values.reshape(seqs, values.shape[0] // seqs, values.shape[1]).transpose(1, 0, 2)

    state_rows = lax.all_gather(state_weight.astype(bf16), "tensor", axis=0, tiled=True)
    full_in = lax.all_gather(normed_in, "tensor", axis=0, tiled=True)
    weights_own = jnp.concatenate(
        [
            inner_weight[0].astype(bf16),
            inner_weight[1].astype(bf16),
            state_rows,
            jnp.pad(step_weight.astype(bf16), ((0, 0), (0, LANES - heads))),
        ],
        axis=1,
    )
    replicas = lax.axis_size("dp")
    gathered = gather_dp(
        jnp.concatenate([weights_own, output_matrix.astype(bf16).T], axis=1), replicas
    )
    cat = weights_own.shape[1]
    weights = gathered[:, :cat]
    output_t = gathered[:, cat:]
    full_cot = lax.all_gather(cotangent, "tensor", axis=0, tiled=True)
    flat_in = by_sequence(full_in)
    flat_cot = by_sequence(full_cot)

    taps = jnp.concatenate([inner_taps, state_taps], axis=1)
    head_rows = jnp.pad(
        jnp.stack([-jnp.exp(head_params[0]), head_params[1]]), ((0, 0), (0, LANES - heads))
    )
    skip = jnp.repeat(head_params[2], size)[None]
    gain = gated_gain[None]
    spread = (jnp.arange(LANES)[:, None] == jnp.arange(wide)[None] // size).astype(bf16)
    gather = (jnp.arange(wide)[:, None] // size == jnp.arange(LANES)[None]).astype(bf16)

    pre = mm(flat_in, weights)
    scanned, conv, gated, chunk_states = run_forward(
        pre, taps, head_rows, skip, spread, seqs, GROUP, size
    )
    d_normed = mm(flat_cot, output_t)
    sums = sum_tensor(
        jnp.stack([jnp.sum(gated * gated, -1), jnp.sum(d_normed * gain * gated, -1)]), shards
    )
    scale_row = lax.rsqrt(sums[0] / inner_total + norm_eps)
    token = jnp.stack([scale_row, scale_row**3 * (sums[1] / inner_total)], axis=1)
    scale = token[:, 0:1]
    normed_out = (gated * scale * gain).astype(bf16)
    branch_part = by_position(mm_nt(normed_out, output_t)).astype(bf16)
    branch_part, d_normed = lax.optimization_barrier((branch_part, d_normed))
    branch = lax.psum_scatter(branch_part, "tensor", scatter_dimension=0, tiled=True)
    result = (base + branch.astype(f32)).astype(bf16)
    output_terms = contract_first(flat_cot, normed_out)

    d_pre, taps_grad, wide_grad, head_grad, grad_output_t = run_backward(
        pre, conv, scanned, d_normed, token, chunk_states, taps, head_rows, skip, gain,
        spread, gather, output_terms, replicas, seqs, GROUP, size,
    )
    d_in_part = mm_nt(d_pre, weights)
    d_in = lax.psum_scatter(
        by_position(d_in_part.astype(bf16)), "tensor", scatter_dimension=0, tiled=True
    ).astype(f32)
    grad_gain_rows = jnp.sum(d_in_part * flat_in.astype(f32), axis=0) / input_gain
    gain_cols = -(-features // (8 * LANES)) * LANES
    small = jnp.concatenate(
        [
            taps_grad,
            wide_grad,
            head_grad,
            jnp.pad(grad_gain_rows, (0, 8 * gain_cols - features)).reshape(8, gain_cols),
        ],
        axis=1,
    )
    grad_own, small_sums, shared_sums, grad_state = sum_dp(
        contract_first(flat_in, d_pre), small, replicas, shards, 2 * wide, states
    )
    taps_grad = small_sums[:, : wide + states]
    wide_grad = small_sums[:, wide + states : 2 * wide + states]
    head_grad = small_sums[:, 2 * wide + states : 2 * wide + states + LANES]
    grad_gain_rows = shared_sums[:, 2 * wide + states + LANES :].reshape(-1)[:features]

    d_hat = d_in * input_gain
    gradient_hidden = cotangent.astype(f32) + rstd * (
        d_hat - normed * jnp.mean(d_hat * normed, -1, keepdims=True)
    )
    grad_skip = jnp.sum(wide_grad[1].reshape(heads, size), axis=1)
    split_terms = (
        taps_grad[: inner_taps.shape[0], :wide],
        jnp.concatenate([head_grad[:2, :heads], grad_skip[None]], axis=0),
        wide_grad[0],
    )
    own = grad_own
    grads = (
        grad_gain_rows,
        jnp.stack([own[:, :wide], own[:, wide : 2 * wide]]),
        own[:, 2 * wide + states : 2 * wide + states + heads],
        grad_state,
        split_terms[0],
        shared_sums[: state_taps.shape[0], wide : wide + states],
        split_terms[1],
        split_terms[2],
        grad_output_t.T,
    )
    stepped = [
        adam_step(param, first, second_moment, grad, rate)
        for param, first, second_moment, grad, rate in zip(params, firsts, seconds, grads, rates)
    ]
    moved = [entry[0] for entry in stepped]
    first_new = [entry[1] for entry in stepped]
    second_new = [entry[2] for entry in stepped]
    return (result, gradient_hidden, *grads, *moved, *first_new, *second_new)


def contract_first(left, right):
    return lax.dot_general(left, right, (((0,), (0,)), ((), ())), preferred_element_type=f32)


def solution(mesh):
    weights = (
        P(),
        P(None, "dp", "tensor"),
        P("dp", "tensor"),
        P(("dp", "tensor"), None),
        P(None, "tensor"),
        P(),
        P(None, "tensor"),
        P("tensor"),
        P("tensor", "dp"),
    )
    rows = P("tensor", "dp", None)

    return jax.shard_map(
        body,
        mesh=mesh,
        in_specs=(rows, rows) + weights * 3,
        out_specs=(rows, rows) + weights * 4,
        check_vma=False,
    )
```

```python
import functools
import jax
import jax.numpy as jnp
from jax import lax
from jax.experimental import pallas as pl
from jax.experimental.pallas import tpu as pltpu
from jax.sharding import PartitionSpec as P

GROUP = 256
norm_eps = 1e-05
beta_first = 0.9
beta_second = 0.95
adam_eps = 1e-08
decay_rate = 0.1
step_count = 4.0
rates = (0.2, 0.008, 0.008, 0.008, 0.1, 0.1, 0.4, 0.2, 0.006)

LANES = 128
CARRY = 8
BLOCKED = -1e30
f32 = jnp.float32
bf16 = jnp.bfloat16


def mm(a, b):
    return lax.dot_general(a, b, (((1,), (0,)), ((), ())), preferred_element_type=f32)


def mm_nt(a, b):
    return lax.dot_general(a, b, (((1,), (1,)), ((), ())), preferred_element_type=f32)


def mm_exact(a, b):
    return lax.dot_general(
        a, b, (((1,), (0,)), ((), ())), precision=lax.Precision.HIGHEST, preferred_element_type=f32
    )


def mm_split(values, weight):
    high = values.astype(bf16)
    low = (values - high.astype(f32)).astype(bf16)
    return mm(high, weight) + mm(low, weight)


MESH = pl.DeviceIdType.MESH
LOADS = 8


def meet(peers, beside=()):
    barrier = pltpu.get_barrier_semaphore()
    for peer in peers:
        pl.semaphore_signal(barrier, inc=1, device_id={"dp": peer}, device_id_type=MESH)
    for peer in beside:
        pl.semaphore_signal(barrier, inc=1, device_id={"tensor": peer}, device_id_type=MESH)
    pl.semaphore_wait(barrier, len(peers) + len(beside))


def send(source, target, send_sem, recv_sem, peer, axis="dp"):
    return pltpu.make_async_remote_copy(
        src_ref=source,
        dst_ref=target,
        send_sem=send_sem,
        recv_sem=recv_sem,
        device_id={axis: peer},
        device_id_type=MESH,
    )


def gather_kernel(n, own_ref, full_ref, own_sem, far_send, far_recv, near_send, near_recv):
    rows = own_ref.shape[0]
    chips = n // 2
    me = lax.axis_index("dp")
    core = lax.rem(me, 2)
    chip = me // 2
    partner = me + 1 - 2 * core
    others = [2 * lax.rem(chip + 1 + k, chips) + core for k in range(chips - 1)]
    meet(others + [partner])

    def place(index):
        return full_ref.at[pl.ds(pl.multiple_of(index * rows, rows), rows), :]

    far = [
        send(own_ref, place(me), far_send.at[k], far_recv.at[k], others[k]) for k in range(chips - 1)
    ]
    for copy in far:
        copy.start()
    near = [send(own_ref, place(me), near_send.at[chips - 1], near_recv.at[chips - 1], partner)]
    near[0].start()
    kept = pltpu.make_async_copy(own_ref, place(me), own_sem)
    kept.start()
    for k in range(chips - 1):
        source = 2 * lax.rem(chip + chips - 1 - k, chips) + core
        far[k].wait_recv()
        copy = send(place(source), place(source), near_send.at[k], near_recv.at[k], partner)
        copy.start()
        near.append(copy)
    kept.wait()
    for copy in far:
        copy.wait_send()
    for copy in near:
        copy.wait()


def gather_dp(own, n):
    rows, cols = own.shape
    return pl.pallas_call(
        functools.partial(gather_kernel, n),
        out_shape=jax.ShapeDtypeStruct((rows * n, cols), own.dtype),
        in_specs=[pl.BlockSpec(memory_space=pltpu.VMEM)],
        out_specs=pl.BlockSpec(memory_space=pl.ANY),
        scratch_shapes=[
            pltpu.SemaphoreType.DMA(()),
            pltpu.SemaphoreType.DMA((n // 2 - 1,)),
            pltpu.SemaphoreType.DMA((n // 2 - 1,)),
            pltpu.SemaphoreType.DMA((n // 2,)),
            pltpu.SemaphoreType.DMA((n // 2,)),
        ],
        compiler_params=pltpu.CompilerParams(collective_id=0, has_side_effects=True),
        cost_estimate=pl.CostEstimate(flops=0, bytes_accessed=240_000_000, transcendentals=0),
        name="gather_dp",
    )(own)


class Exchange:
    def __init__(
        self, n, terms, own_buf, near_buf, out_buf, far_buf, own_sem, near_send, near_recv, far_send, far_recv
    ):
        self.n, self.terms, self.own_buf, self.own_sem = n, terms, own_buf, own_sem
        self.near_buf, self.out_buf, self.far_buf = near_buf, out_buf, far_buf
        self.near_send, self.near_recv, self.far_send, self.far_recv = near_send, near_recv, far_send, far_recv
        self.chips = n // 2
        self.rows = terms.shape[0] // n
        me = lax.axis_index("dp")
        self.core = lax.rem(me, 2)
        self.partner = me + 1 - 2 * self.core
        self.order = [lax.rem(me // 2 + 1 + k, self.chips) for k in range(self.chips)]

    def block(self, index):
        return self.terms.at[pl.ds(pl.multiple_of(index * self.rows, self.rows), self.rows), :]

    def kept(self, k):
        return pltpu.make_async_copy(
            self.block(2 * self.order[k] + self.core), self.own_buf.at[k], self.own_sem.at[k]
        )

    def near(self, k):
        return send(
            self.block(2 * self.order[k] + 1 - self.core), self.near_buf.at[k],
            self.near_send.at[k], self.near_recv.at[k], self.partner,
        )

    def far(self, k):
        return send(
            self.out_buf.at[k], self.far_buf.at[k],
            self.far_send.at[k], self.far_recv.at[k], 2 * self.order[k] + self.core,
        )

    def start_one(self, k):
        self.kept(k).start()
        self.near(k).start()

    def pair_sum(self, k):
        self.kept(k).wait()
        self.near(k).wait()
        return self.own_buf[k] + self.near_buf[k]

    def forward_one(self, k):
        self.out_buf[k] = self.pair_sum(k).astype(bf16)
        self.far(k).start()

    def finish(self):
        total = self.pair_sum(self.chips - 1)
        for k in range(self.chips - 1):
            self.far(k).wait()
            total = total + self.far_buf[k].astype(f32)
        return total

    @staticmethod
    def scratch(n, rows, cols):
        chips = n // 2
        return [
            pltpu.VMEM((chips, rows, cols), f32),
            pltpu.VMEM((chips, rows, cols), f32),
            pltpu.VMEM((chips - 1, rows, cols), bf16),
            pltpu.VMEM((chips - 1, rows, cols), bf16),
            pltpu.SemaphoreType.DMA((chips,)),
            pltpu.SemaphoreType.DMA((chips,)),
            pltpu.SemaphoreType.DMA((chips,)),
            pltpu.SemaphoreType.DMA((chips - 1,)),
            pltpu.SemaphoreType.DMA((chips - 1,)),
        ]


def all_others(n, axis="dp"):
    me = lax.axis_index(axis)
    return [lax.rem(me + 1 + k, n) for k in range(n - 1)]


def sum_kernel(
    n, shards, wide, states, left_hbm, right_hbm, small_ref,
    inner_ref, step_ref, state_ref, taps_ref, wide_ref, head_ref, state_taps_ref, gain_ref,
    left_ref, right_ref, load_sems,
    pair, near_buf, out_buf, far_buf, small_sum, small_buf, state_out, state_buf, shared_buf,
    near_send, near_recv, far_send, far_recv, small_send, small_recv,
    state_send, state_recv, shared_send, shared_recv,
):
    rows, _ = pair.shape[2:]
    chips = n // 2
    loads = []
    for source, target, base in ((right_hbm, right_ref, 0), (left_hbm, left_ref, LOADS)):
        piece = source.shape[0] // LOADS
        for k in range(LOADS):
            part = pl.ds(k * piece, piece)
            loads.append(pltpu.make_async_copy(source.at[part, :], target.at[part, :], load_sems.at[base + k]))
    for load in loads:
        load.start()
    me = lax.axis_index("dp")
    core = lax.rem(me, 2)
    partner = me + 1 - 2 * core
    others = all_others(n)
    beside = all_others(shards, "tensor")
    meet(others, beside)
    copies = [
        send(small_ref, small_buf.at[k], small_send.at[k], small_recv.at[k], others[k])
        for k in range(n - 1)
    ]
    for copy in copies:
        copy.start()

    def chip_of(k):
        return lax.rem(me // 2 + 1 + k, chips)

    def near(k):
        return send(pair.at[k, 1 - core], near_buf.at[k], near_send.at[k], near_recv.at[k], partner)

    def far(k):
        return send(
            out_buf.at[k], far_buf.at[k], far_send.at[k], far_recv.at[k], 2 * chip_of(k) + core
        )

    def product(k):
        start = pl.multiple_of(chip_of(k) * 2 * rows, 2 * rows)
        both = mm(left_ref[pl.ds(start, 2 * rows), :], right_ref[...])
        pair[k, 0] = both[:rows]
        pair[k, 1] = both[rows:]
        near(k).start()

    def step(k, carry):
        product(k + 1)
        near(k).wait()
        out_buf[k] = (pair[k, core] + near_buf[k]).astype(bf16)
        far(k).start()
        return carry

    for load in loads:
        load.wait()
    product(0)
    lax.fori_loop(0, chips - 1, step, 0)
    small = small_ref[...]
    for k in range(n - 1):
        copies[k].wait()
        small = small + small_buf[k]
    small_sum[...] = small
    shared = [
        send(small_sum, shared_buf.at[k], shared_send.at[k], shared_recv.at[k], beside[k], "tensor")
        for k in range(shards - 1)
    ]
    for copy in shared:
        copy.start()
    taps = taps_ref.shape[0]
    taps_ref[...] = small[:taps, :wide]
    wide_ref[...] = small[0:1, wide + states : 2 * wide + states]
    head_ref[...] = small[:, 2 * wide + states : 2 * wide + states + LANES]
    for k in range(shards - 1):
        shared[k].wait()
        small = small + shared_buf[k]
    state_taps_ref[...] = small[:taps, wide : wide + states]
    gain_ref[...] = small[:, 2 * wide + states + LANES :]
    near(chips - 1).wait()
    total = pair[chips - 1, core] + near_buf[chips - 1]
    for k in range(chips - 1):
        far(k).wait()
        total = total + far_buf[k].astype(f32)
    part_rows = state_ref.shape[0]
    for k in range(shards):
        state_out[k] = total[k * part_rows : (k + 1) * part_rows, 2 * wide : 2 * wide + states]
    parts = [
        send(
            state_out.at[beside[k]], state_buf.at[k], state_send.at[k], state_recv.at[k], beside[k], "tensor"
        )
        for k in range(shards - 1)
    ]
    for copy in parts:
        copy.start()
    inner_ref[0] = total[:, :wide]
    inner_ref[1] = total[:, wide : 2 * wide]
    step_ref[...] = total[:, 2 * wide + states :]
    mine = state_out[lax.axis_index("tensor")]
    for k in range(shards - 1):
        parts[k].wait()
        mine = mine + state_buf[k]
    state_ref[...] = mine


def sum_dp(left_t, right, small, n, shards, wide, states, taps):
    rows, cols = left_t.shape[0] // n, right.shape[1]
    chips = n // 2
    part = (rows // shards, states)
    gain_cols = small.shape[1] - 2 * wide - states - LANES
    vmem = pl.BlockSpec(memory_space=pltpu.VMEM)
    shapes = [
        (2, rows, wide), (rows, cols - 2 * wide - states), part, (taps, wide), (1, wide),
        (8, LANES), (taps, states), (8, gain_cols),
    ]
    dma = pltpu.SemaphoreType.DMA
    return pl.pallas_call(
        functools.partial(sum_kernel, n, shards, wide, states),
        out_shape=[jax.ShapeDtypeStruct(shape, f32) for shape in shapes],
        in_specs=[pl.BlockSpec(memory_space=pl.ANY)] * 2 + [vmem],
        out_specs=[vmem] * len(shapes),
        scratch_shapes=[
            pltpu.VMEM(left_t.shape, bf16),
            pltpu.VMEM(right.shape, bf16),
            dma((2 * LOADS,)),
            pltpu.VMEM((chips, 2, rows, cols), f32),
            pltpu.VMEM((chips, rows, cols), f32),
            pltpu.VMEM((chips - 1, rows, cols), bf16),
            pltpu.VMEM((chips - 1, rows, cols), bf16),
            pltpu.VMEM(small.shape, f32),
            pltpu.VMEM((n - 1,) + small.shape, f32),
            pltpu.VMEM((shards,) + part, f32),
            pltpu.VMEM((shards - 1,) + part, f32),
            pltpu.VMEM((shards - 1,) + small.shape, f32),
            dma((chips,)), dma((chips,)), dma((chips - 1,)), dma((chips - 1,)),
            dma((n - 1,)), dma((n - 1,)),
        ]
        + [dma((shards - 1,))] * 4,
        compiler_params=pltpu.CompilerParams(
            collective_id=1, has_side_effects=True, vmem_limit_bytes=60 * 1024 * 1024
        ),
        cost_estimate=pl.CostEstimate(flops=0, bytes_accessed=240_000_000, transcendentals=0),
        name="sum_dp",
    )(left_t, right, small)


def token_kernel(shards, own_ref, total_ref, buf, send_sem, recv_sem):
    beside = all_others(shards, "tensor")
    meet((), beside)
    copies = [
        send(own_ref, buf.at[k], send_sem.at[k], recv_sem.at[k], beside[k], "tensor")
        for k in range(shards - 1)
    ]
    for copy in copies:
        copy.start()
    total = own_ref[...]
    for k in range(shards - 1):
        copies[k].wait()
        total = total + buf[k]
    total_ref[...] = total


def sum_tensor(own, shards):
    vmem = pl.BlockSpec(memory_space=pltpu.VMEM)
    return pl.pallas_call(
        functools.partial(token_kernel, shards),
        out_shape=jax.ShapeDtypeStruct(own.shape, f32),
        in_specs=[vmem],
        out_specs=vmem,
        scratch_shapes=[
            pltpu.VMEM((shards - 1,) + own.shape, f32),
            pltpu.SemaphoreType.DMA((shards - 1,)),
            pltpu.SemaphoreType.DMA((shards - 1,)),
        ],
        compiler_params=pltpu.CompilerParams(collective_id=3, has_side_effects=True),
        name="sum_tensor",
    )(own)


def sigmoid(v):
    return 1.0 / (1.0 + jnp.exp(-v))


def tri_lower(count):
    rows = lax.broadcasted_iota(jnp.int32, (count, count), 0)
    cols = lax.broadcasted_iota(jnp.int32, (count, count), 1)
    return rows >= cols


def step_terms(step_pre, heads_ref):
    shifted = step_pre + heads_ref[1:2, :]
    steps = jnp.maximum(shifted, 0.0) + jnp.log1p(jnp.exp(-jnp.abs(shifted)))
    logs = heads_ref[0:1, :] * steps
    count = logs.shape[0]
    cumul = mm_exact(tri_lower(count).astype(f32), logs)
    return shifted, steps, logs, cumul


def forward_kernel(
    width, size, pre_ref, taps_ref, heads_ref, skip_ref, spread_ref,
    scanned_ref, conv_ref, gated_ref, states_ref,
    ext, state, act,
):
    count = pre_ref.shape[0]
    half = count // 2
    conv_width = taps_ref.shape[1]
    taps = taps_ref.shape[0] - 1
    state_size = (conv_width - width) // 2
    per_tile = LANES // size

    @pl.when(pl.program_id(1) == 0)
    def _():
        ext[0:CARRY, :] = jnp.zeros((CARRY, conv_width), f32)
        state[...] = jnp.zeros_like(state)

    states_ref[0] = state[...]
    for start in range(0, conv_width, LANES):
        cols = slice(start, start + LANES)
        ext[CARRY : CARRY + count, cols] = pre_ref[:, width + start : width + start + LANES]
        total = taps_ref[taps : taps + 1, cols]
        for j in range(taps):
            total = total + taps_ref[j : j + 1, cols] * ext[CARRY + 1 - taps + j : CARRY + 1 - taps + j + count, cols]
        conv_ref[:, cols] = total
        act[:, cols] = total * sigmoid(total)
        ext[0:CARRY, cols] = ext[count : count + CARRY, cols]

    _, steps, _, cumul = step_terms(pre_ref[:, width + conv_width :], heads_ref)
    cumul_t = cumul.T
    final = cumul[count - 1 : count, :]
    decay_in = jnp.exp(cumul)
    decay_out = jnp.exp(final - cumul)
    keys = act[:, width : width + state_size].astype(bf16)
    queries = act[:, width + state_size :].astype(bf16)
    keys_t = act[:, width : width + state_size].T.astype(bf16)
    scores = mm_nt(queries, keys)
    causal = tri_lower(half)
    lane = lax.broadcasted_iota(jnp.int32, (count, LANES), 1)
    for tile in range(width // LANES):
        cols = slice(tile * LANES, (tile + 1) * LANES)
        spread = spread_ref[:, cols]
        inner = act[:, cols]
        scaled = inner * mm_split(steps, spread)
        scaled_b = scaled.astype(bf16)
        mixed = None
        for k in range(per_tile):
            head = tile * per_tile + k
            col = cumul[:, head : head + 1]
            row = cumul_t[head : head + 1, :]
            first = jnp.exp(jnp.where(causal, col[:half] - row[:, :half], BLOCKED)) * scores[:half, :half]
            low = jnp.exp(col[half:] - row[:, :half]) * scores[half:, :half]
            last = jnp.exp(jnp.where(causal, col[half:] - row[:, half:], BLOCKED)) * scores[half:, half:]
            top = mm(first.astype(bf16), scaled_b[:half])
            bottom = mm(jnp.concatenate([low.astype(bf16), last.astype(bf16)], axis=1), scaled_b)
            part = jnp.concatenate([top, bottom], axis=0)
            mixed = part if mixed is None else jnp.where(lane >= k * size, part, mixed)
        in_wide = mm_split(decay_in, spread)
        out_wide = mm_split(decay_out, spread)
        held = state[:, cols]
        scanned = mixed + in_wide * mm(queries, held.astype(bf16))
        state[:, cols] = in_wide[count - 1 : count, :] * held + mm(keys_t, (out_wide * scaled).astype(bf16))
        scanned_ref[:, cols] = scanned
        gate = pre_ref[:, cols]
        gated = (scanned + skip_ref[:, cols] * inner) * (gate * sigmoid(gate))
        gated_ref[:, cols] = gated


def backward_kernel(
    n, blocks, width, size, pre_ref, conv_ref, scanned_ref, dnormed_ref, token_ref, states_ref,
    taps_ref, heads_ref, skip_ref, gain_ref, spread_ref, gather_ref, terms_ref,
    dpre_ref, taps_grad_ref, wide_grad_ref, heads_grad_ref, own_ref,
    ext, dstate, dscores, in_rows, out_rows, dstate_b, finals, *scratch,
):
    exchange = Exchange(n, terms_ref, *scratch)
    opening = (pl.program_id(0) == 0) & (pl.program_id(1) == 0)
    closing = (pl.program_id(0) == pl.num_programs(0) - 1) & (pl.program_id(1) == pl.num_programs(1) - 1)

    @pl.when(opening)
    def _():
        meet(all_others(n))

    far_steps = [1 + k * (blocks - 2) // (exchange.chips - 1) for k in range(exchange.chips - 1)]
    near_steps = [step - 1 for step in far_steps] + [blocks - 2]
    for step in range(blocks - 1):
        fars = [k for k in range(exchange.chips - 1) if far_steps[k] == step]
        nears = [k for k in range(exchange.chips) if near_steps[k] == step]

        @pl.when((pl.program_id(0) == 0) & (pl.program_id(1) == step))
        def _(fars=fars, nears=nears):
            for k in fars:
                exchange.forward_one(k)
            for k in nears:
                exchange.start_one(k)

    count = pre_ref.shape[0]
    half = count // 2
    conv_width = taps_ref.shape[1]
    taps = taps_ref.shape[0] - 1
    state_size = (conv_width - width) // 2
    per_tile = LANES // size

    @pl.when(pl.program_id(1) == 0)
    def _():
        ext[count : count + CARRY, :] = jnp.zeros((CARRY, conv_width), f32)
        dstate[...] = jnp.zeros_like(dstate)

    @pl.when(opening)
    def _():
        taps_grad_ref[...] = jnp.zeros_like(taps_grad_ref)
        wide_grad_ref[...] = jnp.zeros_like(wide_grad_ref)
        heads_grad_ref[...] = jnp.zeros_like(heads_grad_ref)

    shifted, steps, logs, cumul = step_terms(pre_ref[:, width + conv_width :], heads_ref)
    cumul_t = cumul.T
    final = cumul[count - 1 : count, :]
    decay_in = jnp.exp(cumul)
    decay_out = jnp.exp(final - cumul)
    key_cols = slice(width, width + state_size)
    query_cols = slice(width + state_size, conv_width)
    key_pre = conv_ref[:, key_cols]
    query_pre = conv_ref[:, query_cols]
    key_sig = sigmoid(key_pre)
    query_sig = sigmoid(query_pre)
    keys = (key_pre * key_sig).astype(bf16)
    queries = (query_pre * query_sig).astype(bf16)
    queries_t = (query_pre * query_sig).T.astype(bf16)
    scores_t = mm_nt(keys, queries)
    rows = lax.broadcasted_iota(jnp.int32, (half, half), 0)
    columns = lax.broadcasted_iota(jnp.int32, (half, half), 1)
    causal_t = columns >= rows
    lane = lax.broadcasted_iota(jnp.int32, (count, LANES), 1)
    dscores[...] = jnp.zeros_like(dscores)
    scale = token_ref[:, 0:1]
    pull = token_ref[:, 1:2]
    dcumul = jnp.zeros((count, LANES), f32)
    dsteps = jnp.zeros((count, LANES), f32)
    for tile in range(width // LANES):
        cols = slice(tile * LANES, (tile + 1) * LANES)
        spread = spread_ref[:, cols]
        gather = gather_ref[cols, :]
        conv = conv_ref[:, cols]
        sig = sigmoid(conv)
        inner = conv * sig
        gate = pre_ref[:, cols]
        gate_sig = sigmoid(gate)
        gate_act = gate * gate_sig
        scanned = scanned_ref[:, cols]
        mixed = scanned + skip_ref[:, cols] * inner
        gated = mixed * gate_act
        dnormed = dnormed_ref[:, cols]
        wide_grad_ref[0:1, cols] += jnp.sum(dnormed * gated * scale, axis=0, keepdims=True)
        dgated = scale * (dnormed * gain_ref[:, cols]) - pull * gated
        dmixed = dgated * gate_act
        dgate = dgated * mixed * (gate_sig * (1.0 + gate * (1.0 - gate_sig)))
        dpre_ref[:, cols] = dgate.astype(bf16)
        wide_grad_ref[1:2, cols] += jnp.sum(dmixed * inner, axis=0, keepdims=True)
        dmixed_b = dmixed.astype(bf16)
        steps_wide = mm_split(steps, spread)
        scaled = inner * steps_wide
        scaled_b = scaled.astype(bf16)
        dscaled = None
        for k in range(per_tile):
            head = tile * per_tile + k
            col = cumul[:, head : head + 1]
            row = cumul_t[head : head + 1, :]
            own = jnp.where((lane >= k * size) & (lane < (k + 1) * size), scaled, 0.0).astype(bf16)
            first = jnp.exp(jnp.where(causal_t, row[:, :half] - col[:half], BLOCKED))
            right = jnp.exp(row[:, half:] - col[:half])
            last = jnp.exp(jnp.where(causal_t, row[:, half:] - col[half:], BLOCKED))
            top = mm(
                jnp.concatenate(
                    [
                        (first * scores_t[:half, :half]).astype(bf16),
                        (right * scores_t[:half, half:]).astype(bf16),
                    ],
                    axis=1,
                ),
                dmixed_b,
            )
            bottom = mm((last * scores_t[half:, half:]).astype(bf16), dmixed_b[half:])
            part = jnp.concatenate([top, bottom], axis=0)
            dscaled = part if dscaled is None else jnp.where(lane >= k * size, part, dscaled)
            dscores[:half, :half] += mm_nt(own[:half], dmixed_b[:half]) * first
            dscores[:half, half:] += mm_nt(own[:half], dmixed_b[half:]) * right
            dscores[half:, half:] += mm_nt(own[half:], dmixed_b[half:]) * last
        in_wide = mm_split(decay_in, spread)
        out_wide = mm_split(decay_out, spread)
        dheld = dstate[:, cols]
        dheld_b = dheld.astype(bf16)
        dstate_b[:, cols] = dheld_b
        dlate = out_wide * mm(keys, dheld_b)
        dscaled = dscaled + dlate
        rounded = scaled_b.astype(f32)
        dcumul = dcumul + mm_split(dmixed_b.astype(f32) * scanned - rounded * dscaled, gather)
        dsteps = dsteps + mm_split(inner * dscaled, gather)
        final_wide = in_wide[count - 1 : count, :]
        finals[0:1, cols] = jnp.sum(rounded * dlate, axis=0, keepdims=True) + final_wide * jnp.sum(
            dheld * states_ref[0, :, cols], axis=0, keepdims=True
        )
        dinner = dscaled * steps_wide + skip_ref[:, cols] * dmixed
        ext[0:count, cols] = dinner * (sig * (1.0 + conv * (1.0 - sig)))
        in_b = (in_wide * dmixed).astype(bf16)
        in_rows[:, cols] = in_b
        out_rows[:, cols] = (out_wide * scaled).astype(bf16)
        dstate[:, cols] = final_wide * dheld + mm(queries_t, in_b)

    pairs = dscores[...]
    dkeys = mm(pairs.astype(bf16), queries) + mm_nt(out_rows[...], dstate_b[...])
    dqueries = mm(pairs.T.astype(bf16), keys) + mm_nt(in_rows[...], states_ref[0].astype(bf16))
    ext[0:count, key_cols] = dkeys * (key_sig * (1.0 + key_pre * (1.0 - key_sig)))
    ext[0:count, query_cols] = dqueries * (query_sig * (1.0 + query_pre * (1.0 - query_sig)))

    for start in range(0, conv_width, LANES):
        cols = slice(start, start + LANES)
        pre = pre_ref[:, width + start : width + start + LANES]
        total = None
        for j in range(taps):
            moved = ext[taps - 1 - j : taps - 1 - j + count, cols]
            term = taps_ref[j : j + 1, cols] * moved
            total = term if total is None else total + term
            taps_grad_ref[j : j + 1, cols] += jnp.sum(pre * moved, axis=0, keepdims=True)
        taps_grad_ref[taps : taps + 1, cols] += jnp.sum(ext[0:count, cols], axis=0, keepdims=True)
        dpre_ref[:, width + start : width + start + LANES] = total.astype(bf16)
        ext[count : count + CARRY, cols] = ext[0:CARRY, cols]

    final_row = mm_split(jnp.broadcast_to(finals[0:1, :], (CARRY, width)), gather_ref[...])[0:1]
    suffix = 1.0 - tri_lower(count).astype(f32) + jnp.where(
        lax.broadcasted_iota(jnp.int32, (count, count), 0)
        == lax.broadcasted_iota(jnp.int32, (count, count), 1),
        1.0,
        0.0,
    )
    dlogs = mm_exact(suffix, dcumul) + final_row
    dshifted = (dsteps + dlogs * heads_ref[0:1, :]) * sigmoid(shifted)
    dpre_ref[:, width + conv_width :] = dshifted.astype(bf16)
    heads_grad_ref[0:1, :] += jnp.sum(dlogs * logs, axis=0, keepdims=True)
    heads_grad_ref[1:2, :] += jnp.sum(dshifted, axis=0, keepdims=True)

    @pl.when(closing)
    def _():
        own_ref[...] = exchange.finish()
        skips = jnp.broadcast_to(wide_grad_ref[1:2, :], (CARRY, width))
        heads_grad_ref[2:3, :] = mm_split(skips, gather_ref[...])[0:1]


def whole(shape):
    return pl.BlockSpec(shape, lambda s, i: (0,) * len(shape))


def run_forward(pre, taps, heads, skip, spread, seqs, count, size):
    rows, cat = pre.shape
    width = skip.shape[1]
    conv_width = taps.shape[1]
    state_size = (conv_width - width) // 2
    blocks = rows // seqs // count

    def block(cols):
        return pl.BlockSpec((count, cols), lambda s, i: (s * blocks + i, 0))

    return pl.pallas_call(
        functools.partial(forward_kernel, width, size),
        grid=(seqs, blocks),
        in_specs=[block(cat), whole(taps.shape), whole(heads.shape), whole(skip.shape), whole(spread.shape)],
        out_specs=[
            block(width), block(conv_width), block(width),
            pl.BlockSpec((1, state_size, width), lambda s, i: (s * blocks + i, 0, 0)),
        ],
        out_shape=[
            jax.ShapeDtypeStruct((rows, width), f32),
            jax.ShapeDtypeStruct((rows, conv_width), f32),
            jax.ShapeDtypeStruct((rows, width), f32),
            jax.ShapeDtypeStruct((seqs * blocks, state_size, width), f32),
        ],
        scratch_shapes=[
            pltpu.VMEM((count + CARRY, conv_width), f32),
            pltpu.VMEM((state_size, width), f32),
            pltpu.VMEM((count, conv_width), f32),
        ],
        cost_estimate=pl.CostEstimate(
            flops=rows * width * count * 4, bytes_accessed=rows * (cat + 4 * width) * 4, transcendentals=rows * count * 12
        ),
        name="mixer_forward",
    )(pre, taps, heads, skip, spread)


def run_backward(pre, conv, scanned, dnormed, token, states, taps, heads, skip, gain, spread, gather, terms, n, seqs, count, size):
    rows, cat = pre.shape
    width = skip.shape[1]
    conv_width = taps.shape[1]
    state_size = (conv_width - width) // 2
    blocks = rows // seqs // count

    def block(cols):
        return pl.BlockSpec((count, cols), lambda s, i: (s * blocks + blocks - 1 - i, 0))

    return pl.pallas_call(
        functools.partial(backward_kernel, n, blocks, width, size),
        grid=(seqs, blocks),
        in_specs=[
            block(cat), block(conv_width), block(width), block(width), block(2),
            pl.BlockSpec((1, state_size, width), lambda s, i: (s * blocks + blocks - 1 - i, 0, 0)),
            whole(taps.shape), whole(heads.shape), whole(skip.shape), whole(gain.shape),
            whole(spread.shape), whole(gather.shape),
            pl.BlockSpec(memory_space=pl.ANY),
        ],
        out_specs=[
            block(cat), whole((8, conv_width)), whole((8, width)), whole((8, LANES)),
            whole((terms.shape[0] // n, terms.shape[1])),
        ],
        out_shape=[
            jax.ShapeDtypeStruct((rows, cat), bf16),
            jax.ShapeDtypeStruct((8, conv_width), f32),
            jax.ShapeDtypeStruct((8, width), f32),
            jax.ShapeDtypeStruct((8, LANES), f32),
            jax.ShapeDtypeStruct((terms.shape[0] // n, terms.shape[1]), f32),
        ],
        scratch_shapes=[
            pltpu.VMEM((count + CARRY, conv_width), f32),
            pltpu.VMEM((state_size, width), f32),
            pltpu.VMEM((count, count), f32),
            pltpu.VMEM((count, width), bf16),
            pltpu.VMEM((count, width), bf16),
            pltpu.VMEM((state_size, width), bf16),
            pltpu.VMEM((8, width), f32),
        ]
        + Exchange.scratch(n, terms.shape[0] // n, terms.shape[1]),
        compiler_params=pltpu.CompilerParams(
            collective_id=2, has_side_effects=True, vmem_limit_bytes=56 * 1024 * 1024
        ),
        cost_estimate=pl.CostEstimate(
            flops=rows * width * count * 8, bytes_accessed=rows * (2 * cat + 4 * width) * 4, transcendentals=rows * count * 12
        ),
        name="mixer_backward",
    )(pre, conv, scanned, dnormed, token, states, taps, heads, skip, gain, spread, gather, terms)


def adam_step(param, first, second_moment, grad, rate):
    first_new = beta_first * first + (1.0 - beta_first) * grad
    second_new = beta_second * second_moment + (1.0 - beta_second) * grad * grad
    first_hat = first_new / (1.0 - beta_first**step_count)
    second_hat = second_new / (1.0 - beta_second**step_count)
    moved = param - rate * (first_hat / (jnp.sqrt(second_hat) + adam_eps) + decay_rate * param)
    return (moved, first_new, second_new)


def body(hidden, cotangent, *arrays):
    params, firsts, seconds = arrays[:9], arrays[9:18], arrays[18:27]
    (
        input_gain,
        inner_weight,
        step_weight,
        state_weight,
        inner_taps,
        state_taps,
        head_params,
        gated_gain,
        output_matrix,
    ) = params
    _, seqs, features = hidden.shape
    wide = inner_taps.shape[1]
    heads = head_params.shape[1]
    size = wide // heads
    states = state_taps.shape[1]
    shards = lax.axis_size("tensor")
    inner_total = wide * shards

    base = hidden.astype(f32)
    rstd = lax.rsqrt(jnp.mean(base * base, -1, keepdims=True) + norm_eps)
    normed = base * rstd
    normed_in = (normed * input_gain).astype(bf16)

    def by_sequence(values):
        return values.transpose(1, 0, 2).reshape(values.shape[0] * seqs, values.shape[2])

    def by_position(values):
        return values.reshape(seqs, values.shape[0] // seqs, values.shape[1]).transpose(1, 0, 2)

    state_rows = lax.all_gather(state_weight.astype(bf16), "tensor", axis=0, tiled=True)
    full_in = lax.all_gather(normed_in, "tensor", axis=0, tiled=True)
    weights_own = jnp.concatenate(
        [
            inner_weight[0].astype(bf16),
            inner_weight[1].astype(bf16),
            state_rows,
            jnp.pad(step_weight.astype(bf16), ((0, 0), (0, LANES - heads))),
        ],
        axis=1,
    )
    replicas = lax.axis_size("dp")
    gathered = gather_dp(
        jnp.concatenate([weights_own, output_matrix.astype(bf16).T], axis=1), replicas
    )
    cat = weights_own.shape[1]
    weights = gathered[:, :cat]
    output_t = gathered[:, cat:]
    full_cot = lax.all_gather(cotangent, "tensor", axis=0, tiled=True)
    flat_in = by_sequence(full_in)
    flat_cot = by_sequence(full_cot)

    taps = jnp.concatenate([inner_taps, state_taps], axis=1)
    head_rows = jnp.pad(
        jnp.stack([-jnp.exp(head_params[0]), head_params[1]]), ((0, 0), (0, LANES - heads))
    )
    skip = jnp.repeat(head_params[2], size)[None]
    gain = gated_gain[None]
    spread = (jnp.arange(LANES)[:, None] == jnp.arange(wide)[None] // size).astype(bf16)
    gather = (jnp.arange(wide)[:, None] // size == jnp.arange(LANES)[None]).astype(bf16)

    pre = mm(flat_in, weights)
    scanned, conv, gated, chunk_states = run_forward(
        pre, taps, head_rows, skip, spread, seqs, GROUP, size
    )
    d_normed = mm(flat_cot, output_t)
    sums = sum_tensor(
        jnp.stack([jnp.sum(gated * gated, -1), jnp.sum(d_normed * gain * gated, -1)]), shards
    )
    scale_row = lax.rsqrt(sums[0] / inner_total + norm_eps)
    token = jnp.stack([scale_row, scale_row**3 * (sums[1] / inner_total)], axis=1)
    scale = token[:, 0:1]
    normed_out = (gated * scale * gain).astype(bf16)
    branch_part = by_position(mm_nt(normed_out, output_t)).astype(bf16)
    branch_part, d_normed = lax.optimization_barrier((branch_part, d_normed))
    branch = lax.psum_scatter(branch_part, "tensor", scatter_dimension=0, tiled=True)
    result = (base + branch.astype(f32)).astype(bf16)
    output_terms = contract_first(flat_cot, normed_out)

    d_pre, taps_grad, wide_grad, head_grad, grad_output_t = run_backward(
        pre, conv, scanned, d_normed, token, chunk_states, taps, head_rows, skip, gain,
        spread, gather, output_terms, replicas, seqs, GROUP, size,
    )
    d_in_part = mm_nt(d_pre, weights)
    d_in = lax.psum_scatter(
        by_position(d_in_part.astype(bf16)), "tensor", scatter_dimension=0, tiled=True
    ).astype(f32)
    grad_gain_rows = jnp.sum(d_in_part * flat_in.astype(f32), axis=0) / input_gain
    gain_cols = -(-features // (8 * LANES)) * LANES
    small = jnp.concatenate(
        [
            taps_grad,
            wide_grad,
            head_grad,
            jnp.pad(grad_gain_rows, (0, 8 * gain_cols - features)).reshape(8, gain_cols),
        ],
        axis=1,
    )
    grad_inner, step_sums, grad_state, grad_taps, grad_wide, head_sums, grad_state_taps, gain_sums = sum_dp(
        flat_in.T, d_pre, small, replicas, shards, wide, states, inner_taps.shape[0]
    )
    grad_output = grad_output_t.T

    d_hat = d_in * input_gain
    gradient_hidden = cotangent.astype(f32) + rstd * (
        d_hat - normed * jnp.mean(d_hat * normed, -1, keepdims=True)
    )
    grads = (
        gain_sums.reshape(-1)[:features],
        grad_inner,
        step_sums[:, :heads],
        grad_state,
        grad_taps,
        grad_state_taps,
        head_sums[:3, :heads],
        grad_wide[0],
        grad_output,
    )
    stepped = [
        adam_step(param, first, second_moment, grad, rate)
        for param, first, second_moment, grad, rate in zip(params, firsts, seconds, grads, rates)
    ]
    moved = [entry[0] for entry in stepped]
    first_new = [entry[1] for entry in stepped]
    second_new = [entry[2] for entry in stepped]
    return (result, gradient_hidden, *grads, *moved, *first_new, *second_new)


def contract_first(left, right):
    return lax.dot_general(left, right, (((0,), (0,)), ((), ())), preferred_element_type=f32)


def solution(mesh):
    weights = (
        P(),
        P(None, "dp", "tensor"),
        P("dp", "tensor"),
        P(("dp", "tensor"), None),
        P(None, "tensor"),
        P(),
        P(None, "tensor"),
        P("tensor"),
        P("tensor", "dp"),
    )
    rows = P("tensor", "dp", None)

    return jax.shard_map(
        body,
        mesh=mesh,
        in_specs=(rows, rows) + weights * 3,
        out_specs=(rows, rows) + weights * 4,
        check_vma=False,
    )
```

```python
import functools
import jax
import jax.numpy as jnp
from jax import lax
from jax.experimental import pallas as pl
from jax.experimental.pallas import tpu as pltpu
from jax.sharding import PartitionSpec as P

GROUP = 256
norm_eps = 1e-05
beta_first = 0.9
beta_second = 0.95
adam_eps = 1e-08
decay_rate = 0.1
step_count = 4.0
rates = (0.2, 0.008, 0.008, 0.008, 0.1, 0.1, 0.4, 0.2, 0.006)

LANES = 128
CARRY = 8
BLOCKED = -1e30
f32 = jnp.float32
bf16 = jnp.bfloat16


def mm(a, b):
    return lax.dot_general(a, b, (((1,), (0,)), ((), ())), preferred_element_type=f32)


def mm_nt(a, b):
    return lax.dot_general(a, b, (((1,), (1,)), ((), ())), preferred_element_type=f32)


def mm_exact(a, b):
    return lax.dot_general(
        a, b, (((1,), (0,)), ((), ())), precision=lax.Precision.HIGHEST, preferred_element_type=f32
    )


def mm_split(values, weight):
    high = values.astype(bf16)
    low = (values - high.astype(f32)).astype(bf16)
    return mm(high, weight) + mm(low, weight)


MESH = pl.DeviceIdType.MESH
LOADS = 8


def meet(peers, beside=()):
    barrier = pltpu.get_barrier_semaphore()
    for peer in peers:
        pl.semaphore_signal(barrier, inc=1, device_id={"dp": peer}, device_id_type=MESH)
    for peer in beside:
        pl.semaphore_signal(barrier, inc=1, device_id={"tensor": peer}, device_id_type=MESH)
    pl.semaphore_wait(barrier, len(peers) + len(beside))


def send(source, target, send_sem, recv_sem, peer, axis="dp"):
    return pltpu.make_async_remote_copy(
        src_ref=source,
        dst_ref=target,
        send_sem=send_sem,
        recv_sem=recv_sem,
        device_id={axis: peer},
        device_id_type=MESH,
    )


def gather_kernel(
    n, own_ref, full_ref, own_sem, right_send, right_recv, left_send, left_recv, near_send, near_recv
):
    rows = own_ref.shape[0]
    chips = n // 2
    me = lax.axis_index("dp")
    core = lax.rem(me, 2)
    chip = me // 2
    partner = me + 1 - 2 * core
    meet([2 * lax.rem(chip + 1 + k, chips) + core for k in range(chips - 1)] + [partner])

    def place(index):
        return full_ref.at[pl.ds(pl.multiple_of(index * rows, rows), rows), :]

    def right(k):
        source = me - 2 * k
        return send(
            own_ref if k == 0 else place(source), place(source), right_send.at[k], right_recv.at[k],
            lax.rem(me + 2, n),
        )

    def left(k):
        source = me + 2 * k
        return send(
            own_ref if k == 0 else place(source), place(source), left_send.at[k], left_recv.at[k],
            lax.rem(me + n - 2, n),
        )

    def near(source, k):
        return send(
            own_ref if k == 0 else place(source), place(source), near_send.at[k], near_recv.at[k], partner
        )

    def sends_right(k):
        return (chip >= k) & (chip < chips - 1)

    def sends_left(k):
        return (chip + k < chips) & (chip > 0)

    kept = pltpu.make_async_copy(own_ref, place(me), own_sem)
    for k in range(chips - 1):

        @pl.when(sends_right(k))
        def _():
            right(k).start()

        @pl.when(sends_left(k))
        def _():
            left(k).start()

        if k == 0:
            near(me, 0).start()
            kept.start()

        @pl.when(chip >= k + 1)
        def _():
            right(k).wait_recv()
            near(me - 2 * (k + 1), 1 + k).start()

        @pl.when(chip + k + 1 < chips)
        def _():
            left(k).wait_recv()
            near(me + 2 * (k + 1), chips + k).start()

    kept.wait()
    near(me, 0).wait()
    for k in range(chips - 1):

        @pl.when(sends_right(k))
        def _():
            right(k).wait_send()

        @pl.when(sends_left(k))
        def _():
            left(k).wait_send()

        @pl.when(chip >= k + 1)
        def _():
            near(me - 2 * (k + 1), 1 + k).wait()

        @pl.when(chip + k + 1 < chips)
        def _():
            near(me + 2 * (k + 1), chips + k).wait()


def gather_dp(own, n):
    rows, cols = own.shape
    hops = n // 2 - 1
    return pl.pallas_call(
        functools.partial(gather_kernel, n),
        out_shape=jax.ShapeDtypeStruct((rows * n, cols), own.dtype),
        in_specs=[pl.BlockSpec(memory_space=pltpu.VMEM)],
        out_specs=pl.BlockSpec(memory_space=pl.ANY),
        scratch_shapes=[pltpu.SemaphoreType.DMA(())]
        + [pltpu.SemaphoreType.DMA((hops,))] * 4
        + [pltpu.SemaphoreType.DMA((2 * hops + 1,))] * 2,
        compiler_params=pltpu.CompilerParams(collective_id=0, has_side_effects=True),
        cost_estimate=pl.CostEstimate(flops=0, bytes_accessed=240_000_000, transcendentals=0),
        name="gather_dp",
    )(own)


class Exchange:
    def __init__(
        self, n, terms, own_buf, near_buf, out_buf, far_buf, own_sem, near_send, near_recv, far_send, far_recv
    ):
        self.n, self.terms, self.own_buf, self.own_sem = n, terms, own_buf, own_sem
        self.near_buf, self.out_buf, self.far_buf = near_buf, out_buf, far_buf
        self.near_send, self.near_recv, self.far_send, self.far_recv = near_send, near_recv, far_send, far_recv
        self.chips = n // 2
        self.rows = terms.shape[0] // n
        me = lax.axis_index("dp")
        self.core = lax.rem(me, 2)
        self.partner = me + 1 - 2 * self.core
        self.order = [lax.rem(me // 2 + 1 + k, self.chips) for k in range(self.chips)]

    def block(self, index):
        return self.terms.at[pl.ds(pl.multiple_of(index * self.rows, self.rows), self.rows), :]

    def kept(self, k):
        return pltpu.make_async_copy(
            self.block(2 * self.order[k] + self.core), self.own_buf.at[k], self.own_sem.at[k]
        )

    def near(self, k):
        return send(
            self.block(2 * self.order[k] + 1 - self.core), self.near_buf.at[k],
            self.near_send.at[k], self.near_recv.at[k], self.partner,
        )

    def far(self, k):
        return send(
            self.out_buf.at[k], self.far_buf.at[k],
            self.far_send.at[k], self.far_recv.at[k], 2 * self.order[k] + self.core,
        )

    def start_one(self, k):
        self.kept(k).start()
        self.near(k).start()

    def pair_sum(self, k):
        self.kept(k).wait()
        self.near(k).wait()
        return self.own_buf[k] + self.near_buf[k]

    def forward_one(self, k):
        self.out_buf[k] = self.pair_sum(k).astype(bf16)
        self.far(k).start()

    def finish(self):
        total = self.pair_sum(self.chips - 1)
        for k in range(self.chips - 1):
            self.far(k).wait()
            total = total + self.far_buf[k].astype(f32)
        return total

    @staticmethod
    def scratch(n, rows, cols):
        chips = n // 2
        return [
            pltpu.VMEM((chips, rows, cols), f32),
            pltpu.VMEM((chips, rows, cols), f32),
            pltpu.VMEM((chips - 1, rows, cols), bf16),
            pltpu.VMEM((chips - 1, rows, cols), bf16),
            pltpu.SemaphoreType.DMA((chips,)),
            pltpu.SemaphoreType.DMA((chips,)),
            pltpu.SemaphoreType.DMA((chips,)),
            pltpu.SemaphoreType.DMA((chips - 1,)),
            pltpu.SemaphoreType.DMA((chips - 1,)),
        ]


def all_others(n, axis="dp"):
    me = lax.axis_index(axis)
    return [lax.rem(me + 1 + k, n) for k in range(n - 1)]


def sum_kernel(
    n, shards, wide, states, left_hbm, right_hbm, small_ref,
    inner_ref, step_ref, state_ref, taps_ref, wide_ref, head_ref, state_taps_ref, gain_ref,
    left_ref, right_ref, load_sems,
    pair, near_buf, out_buf, far_buf, small_sum, small_buf, state_out, state_buf, shared_buf,
    near_send, near_recv, far_send, far_recv, small_send, small_recv,
    state_send, state_recv, shared_send, shared_recv,
):
    rows, _ = pair.shape[2:]
    chips = n // 2
    loads = []
    for source, target, base in ((right_hbm, right_ref, 0), (left_hbm, left_ref, LOADS)):
        piece = source.shape[0] // LOADS
        for k in range(LOADS):
            part = pl.ds(k * piece, piece)
            loads.append(pltpu.make_async_copy(source.at[part, :], target.at[part, :], load_sems.at[base + k]))
    for load in loads:
        load.start()
    me = lax.axis_index("dp")
    core = lax.rem(me, 2)
    partner = me + 1 - 2 * core
    others = all_others(n)
    beside = all_others(shards, "tensor")
    meet(others, beside)
    copies = [
        send(small_ref, small_buf.at[k], small_send.at[k], small_recv.at[k], others[k])
        for k in range(n - 1)
    ]
    for copy in copies:
        copy.start()

    def chip_of(k):
        return lax.rem(me // 2 + 1 + k, chips)

    def near(k):
        return send(pair.at[k, 1 - core], near_buf.at[k], near_send.at[k], near_recv.at[k], partner)

    def far(k):
        return send(
            out_buf.at[k], far_buf.at[k], far_send.at[k], far_recv.at[k], 2 * chip_of(k) + core
        )

    def product(k):
        start = pl.multiple_of(chip_of(k) * 2 * rows, 2 * rows)
        both = mm(left_ref[pl.ds(start, 2 * rows), :], right_ref[...])
        pair[k, 0] = both[:rows]
        pair[k, 1] = both[rows:]
        near(k).start()

    def step(k, carry):
        product(k)

        @pl.when(k > 0)
        def _():
            near(k - 1).wait()
            out_buf[k - 1] = (pair[k - 1, core] + near_buf[k - 1]).astype(bf16)
            far(k - 1).start()

        return carry

    for load in loads:
        load.wait()
    lax.fori_loop(0, chips, step, 0)
    small = small_ref[...]
    for k in range(n - 1):
        copies[k].wait()
        small = small + small_buf[k]
    small_sum[...] = small
    shared = [
        send(small_sum, shared_buf.at[k], shared_send.at[k], shared_recv.at[k], beside[k], "tensor")
        for k in range(shards - 1)
    ]
    for copy in shared:
        copy.start()
    taps = taps_ref.shape[0]
    taps_ref[...] = small[:taps, :wide]
    wide_ref[...] = small[0:1, wide + states : 2 * wide + states]
    head_ref[...] = small[:, 2 * wide + states : 2 * wide + states + LANES]
    for k in range(shards - 1):
        shared[k].wait()
        small = small + shared_buf[k]
    state_taps_ref[...] = small[:taps, wide : wide + states]
    gain_ref[...] = small[:, 2 * wide + states + LANES :]
    near(chips - 1).wait()
    total = pair[chips - 1, core] + near_buf[chips - 1]
    for k in range(chips - 1):
        far(k).wait()
        total = total + far_buf[k].astype(f32)
    part_rows = state_ref.shape[0]
    for k in range(shards):
        state_out[k] = total[k * part_rows : (k + 1) * part_rows, 2 * wide : 2 * wide + states]
    parts = [
        send(
            state_out.at[beside[k]], state_buf.at[k], state_send.at[k], state_recv.at[k], beside[k], "tensor"
        )
        for k in range(shards - 1)
    ]
    for copy in parts:
        copy.start()
    inner_ref[0] = total[:, :wide]
    inner_ref[1] = total[:, wide : 2 * wide]
    spare = jnp.zeros((-rows % LANES, LANES), f32)
    step_ref[...] = jnp.concatenate([total[:, 2 * wide + states :], spare], axis=0).T[:, :rows]
    mine = state_out[lax.axis_index("tensor")]
    for k in range(shards - 1):
        parts[k].wait()
        mine = mine + state_buf[k]
    state_ref[...] = mine


def sum_dp(left_t, right, small, n, shards, wide, states, taps):
    rows, cols = left_t.shape[0] // n, right.shape[1]
    chips = n // 2
    part = (rows // shards, states)
    gain_cols = small.shape[1] - 2 * wide - states - LANES
    vmem = pl.BlockSpec(memory_space=pltpu.VMEM)
    shapes = [
        (2, rows, wide), (LANES, rows), part, (taps, wide), (1, wide),
        (8, LANES), (taps, states), (8, gain_cols),
    ]
    dma = pltpu.SemaphoreType.DMA
    return pl.pallas_call(
        functools.partial(sum_kernel, n, shards, wide, states),
        out_shape=[jax.ShapeDtypeStruct(shape, f32) for shape in shapes],
        in_specs=[pl.BlockSpec(memory_space=pl.ANY)] * 2 + [vmem],
        out_specs=[vmem] * len(shapes),
        scratch_shapes=[
            pltpu.VMEM(left_t.shape, bf16),
            pltpu.VMEM(right.shape, bf16),
            dma((2 * LOADS,)),
            pltpu.VMEM((chips, 2, rows, cols), f32),
            pltpu.VMEM((chips, rows, cols), f32),
            pltpu.VMEM((chips - 1, rows, cols), bf16),
            pltpu.VMEM((chips - 1, rows, cols), bf16),
            pltpu.VMEM(small.shape, f32),
            pltpu.VMEM((n - 1,) + small.shape, f32),
            pltpu.VMEM((shards,) + part, f32),
            pltpu.VMEM((shards - 1,) + part, f32),
            pltpu.VMEM((shards - 1,) + small.shape, f32),
            dma((chips,)), dma((chips,)), dma((chips - 1,)), dma((chips - 1,)),
            dma((n - 1,)), dma((n - 1,)),
        ]
        + [dma((shards - 1,))] * 4,
        compiler_params=pltpu.CompilerParams(
            collective_id=1, has_side_effects=True, vmem_limit_bytes=60 * 1024 * 1024
        ),
        cost_estimate=pl.CostEstimate(flops=0, bytes_accessed=240_000_000, transcendentals=0),
        name="sum_dp",
    )(left_t, right, small)


def token_kernel(shards, own_ref, total_ref, buf, send_sem, recv_sem):
    beside = all_others(shards, "tensor")
    meet((), beside)
    copies = [
        send(own_ref, buf.at[k], send_sem.at[k], recv_sem.at[k], beside[k], "tensor")
        for k in range(shards - 1)
    ]
    for copy in copies:
        copy.start()
    total = own_ref[...]
    for k in range(shards - 1):
        copies[k].wait()
        total = total + buf[k]
    total_ref[...] = total


def sum_tensor(own, shards):
    vmem = pl.BlockSpec(memory_space=pltpu.VMEM)
    return pl.pallas_call(
        functools.partial(token_kernel, shards),
        out_shape=jax.ShapeDtypeStruct(own.shape, f32),
        in_specs=[vmem],
        out_specs=vmem,
        scratch_shapes=[
            pltpu.VMEM((shards - 1,) + own.shape, f32),
            pltpu.SemaphoreType.DMA((shards - 1,)),
            pltpu.SemaphoreType.DMA((shards - 1,)),
        ],
        compiler_params=pltpu.CompilerParams(collective_id=3, has_side_effects=True),
        name="sum_tensor",
    )(own)


def spread_kernel(shards, own_ref, full_ref, send_sem, recv_sem):
    beside = all_others(shards, "tensor")
    me = lax.axis_index("tensor")
    meet((), beside)
    copies = [
        send(own_ref, full_ref.at[me], send_sem.at[k], recv_sem.at[k], beside[k], "tensor")
        for k in range(shards - 1)
    ]
    for copy in copies:
        copy.start()
    full_ref[me] = own_ref[...]
    for copy in copies:
        copy.wait()


def gather_tensor(own, shards):
    vmem = pl.BlockSpec(memory_space=pltpu.VMEM)
    return pl.pallas_call(
        functools.partial(spread_kernel, shards),
        out_shape=jax.ShapeDtypeStruct((shards,) + own.shape, own.dtype),
        in_specs=[vmem],
        out_specs=vmem,
        scratch_shapes=[
            pltpu.SemaphoreType.DMA((shards - 1,)),
            pltpu.SemaphoreType.DMA((shards - 1,)),
        ],
        compiler_params=pltpu.CompilerParams(collective_id=4, has_side_effects=True),
        name="gather_tensor",
    )(own)


def sigmoid(v):
    return 1.0 / (1.0 + jnp.exp(-v))


def tri_lower(count):
    rows = lax.broadcasted_iota(jnp.int32, (count, count), 0)
    cols = lax.broadcasted_iota(jnp.int32, (count, count), 1)
    return rows >= cols


def step_terms(step_pre, heads_ref):
    shifted = step_pre + heads_ref[1:2, :]
    steps = jnp.maximum(shifted, 0.0) + jnp.log1p(jnp.exp(-jnp.abs(shifted)))
    logs = heads_ref[0:1, :] * steps
    count = logs.shape[0]
    cumul = mm_exact(tri_lower(count).astype(f32), logs)
    return shifted, steps, logs, cumul


def forward_kernel(
    width, size, pre_ref, taps_ref, heads_ref, skip_ref, spread_ref,
    scanned_ref, conv_ref, gated_ref, states_ref,
    ext, state, act,
):
    count = pre_ref.shape[0]
    half = count // 2
    conv_width = taps_ref.shape[1]
    taps = taps_ref.shape[0] - 1
    state_size = (conv_width - width) // 2
    per_tile = LANES // size

    @pl.when(pl.program_id(1) == 0)
    def _():
        ext[0:CARRY, :] = jnp.zeros((CARRY, conv_width), f32)
        state[...] = jnp.zeros_like(state)

    states_ref[0] = state[...]
    for start in range(0, conv_width, LANES):
        cols = slice(start, start + LANES)
        ext[CARRY : CARRY + count, cols] = pre_ref[:, width + start : width + start + LANES]
        total = taps_ref[taps : taps + 1, cols]
        for j in range(taps):
            total = total + taps_ref[j : j + 1, cols] * ext[CARRY + 1 - taps + j : CARRY + 1 - taps + j + count, cols]
        conv_ref[:, cols] = total
        act[:, cols] = total * sigmoid(total)
        ext[0:CARRY, cols] = ext[count : count + CARRY, cols]

    _, steps, _, cumul = step_terms(pre_ref[:, width + conv_width :], heads_ref)
    cumul_t = cumul.T
    final = cumul[count - 1 : count, :]
    decay_in = jnp.exp(cumul)
    decay_out = jnp.exp(final - cumul)
    keys = act[:, width : width + state_size].astype(bf16)
    queries = act[:, width + state_size :].astype(bf16)
    keys_t = act[:, width : width + state_size].T.astype(bf16)
    scores = mm_nt(queries, keys)
    causal = tri_lower(half)
    lane = lax.broadcasted_iota(jnp.int32, (count, LANES), 1)
    for tile in range(width // LANES):
        cols = slice(tile * LANES, (tile + 1) * LANES)
        spread = spread_ref[:, cols]
        inner = act[:, cols]
        scaled = inner * mm_split(steps, spread)
        scaled_b = scaled.astype(bf16)
        mixed = None
        for k in range(per_tile):
            head = tile * per_tile + k
            col = cumul[:, head : head + 1]
            row = cumul_t[head : head + 1, :]
            first = jnp.exp(jnp.where(causal, col[:half] - row[:, :half], BLOCKED)) * scores[:half, :half]
            low = jnp.exp(col[half:] - row[:, :half]) * scores[half:, :half]
            last = jnp.exp(jnp.where(causal, col[half:] - row[:, half:], BLOCKED)) * scores[half:, half:]
            top = mm(first.astype(bf16), scaled_b[:half])
            bottom = mm(jnp.concatenate([low.astype(bf16), last.astype(bf16)], axis=1), scaled_b)
            part = jnp.concatenate([top, bottom], axis=0)
            mixed = part if mixed is None else jnp.where(lane >= k * size, part, mixed)
        in_wide = mm_split(decay_in, spread)
        out_wide = mm_split(decay_out, spread)
        held = state[:, cols]
        scanned = mixed + in_wide * mm(queries, held.astype(bf16))
        state[:, cols] = in_wide[count - 1 : count, :] * held + mm(keys_t, (out_wide * scaled).astype(bf16))
        scanned_ref[:, cols] = scanned
        gate = pre_ref[:, cols]
        gated = (scanned + skip_ref[:, cols] * inner) * (gate * sigmoid(gate))
        gated_ref[:, cols] = gated


def backward_kernel(
    n, blocks, width, size, pre_ref, conv_ref, scanned_ref, dnormed_ref, token_ref, states_ref,
    taps_ref, heads_ref, skip_ref, gain_ref, spread_ref, gather_ref, terms_ref,
    dpre_ref, taps_grad_ref, wide_grad_ref, heads_grad_ref, own_ref,
    ext, dstate, dscores, in_rows, out_rows, dstate_b, finals, *scratch,
):
    exchange = Exchange(n, terms_ref, *scratch)
    opening = (pl.program_id(0) == 0) & (pl.program_id(1) == 0)
    closing = (pl.program_id(0) == pl.num_programs(0) - 1) & (pl.program_id(1) == pl.num_programs(1) - 1)

    @pl.when(opening)
    def _():
        meet(all_others(n))

    far_steps = [1 + k * (blocks - 2) // (exchange.chips - 1) for k in range(exchange.chips - 1)]
    near_steps = [step - 1 for step in far_steps] + [blocks - 2]
    for step in range(blocks - 1):
        fars = [k for k in range(exchange.chips - 1) if far_steps[k] == step]
        nears = [k for k in range(exchange.chips) if near_steps[k] == step]

        @pl.when((pl.program_id(0) == 0) & (pl.program_id(1) == step))
        def _(fars=fars, nears=nears):
            for k in fars:
                exchange.forward_one(k)
            for k in nears:
                exchange.start_one(k)

    count = pre_ref.shape[0]
    half = count // 2
    conv_width = taps_ref.shape[1]
    taps = taps_ref.shape[0] - 1
    state_size = (conv_width - width) // 2
    per_tile = LANES // size

    @pl.when(pl.program_id(1) == 0)
    def _():
        ext[count : count + CARRY, :] = jnp.zeros((CARRY, conv_width), f32)
        dstate[...] = jnp.zeros_like(dstate)

    @pl.when(opening)
    def _():
        taps_grad_ref[...] = jnp.zeros_like(taps_grad_ref)
        wide_grad_ref[...] = jnp.zeros_like(wide_grad_ref)
        heads_grad_ref[...] = jnp.zeros_like(heads_grad_ref)

    shifted, steps, logs, cumul = step_terms(pre_ref[:, width + conv_width :], heads_ref)
    cumul_t = cumul.T
    final = cumul[count - 1 : count, :]
    decay_in = jnp.exp(cumul)
    decay_out = jnp.exp(final - cumul)
    key_cols = slice(width, width + state_size)
    query_cols = slice(width + state_size, conv_width)
    key_pre = conv_ref[:, key_cols]
    query_pre = conv_ref[:, query_cols]
    key_sig = sigmoid(key_pre)
    query_sig = sigmoid(query_pre)
    keys = (key_pre * key_sig).astype(bf16)
    queries = (query_pre * query_sig).astype(bf16)
    queries_t = (query_pre * query_sig).T.astype(bf16)
    scores_t = mm_nt(keys, queries)
    rows = lax.broadcasted_iota(jnp.int32, (half, half), 0)
    columns = lax.broadcasted_iota(jnp.int32, (half, half), 1)
    causal_t = columns >= rows
    lane = lax.broadcasted_iota(jnp.int32, (count, LANES), 1)
    dscores[...] = jnp.zeros_like(dscores)
    scale = token_ref[:, 0:1]
    pull = token_ref[:, 1:2]
    dcumul = jnp.zeros((count, LANES), f32)
    dsteps = jnp.zeros((count, LANES), f32)
    for tile in range(width // LANES):
        cols = slice(tile * LANES, (tile + 1) * LANES)
        spread = spread_ref[:, cols]
        gather = gather_ref[cols, :]
        conv = conv_ref[:, cols]
        sig = sigmoid(conv)
        inner = conv * sig
        gate = pre_ref[:, cols]
        gate_sig = sigmoid(gate)
        gate_act = gate * gate_sig
        scanned = scanned_ref[:, cols]
        mixed = scanned + skip_ref[:, cols] * inner
        gated = mixed * gate_act
        dnormed = dnormed_ref[:, cols]
        wide_grad_ref[0:1, cols] += jnp.sum(dnormed * gated * scale, axis=0, keepdims=True)
        dgated = scale * (dnormed * gain_ref[:, cols]) - pull * gated
        dmixed = dgated * gate_act
        dgate = dgated * mixed * (gate_sig * (1.0 + gate * (1.0 - gate_sig)))
        dpre_ref[:, cols] = dgate.astype(bf16)
        wide_grad_ref[1:2, cols] += jnp.sum(dmixed * inner, axis=0, keepdims=True)
        dmixed_b = dmixed.astype(bf16)
        steps_wide = mm_split(steps, spread)
        scaled = inner * steps_wide
        scaled_b = scaled.astype(bf16)
        dscaled = None
        for k in range(per_tile):
            head = tile * per_tile + k
            col = cumul[:, head : head + 1]
            row = cumul_t[head : head + 1, :]
            own = jnp.where((lane >= k * size) & (lane < (k + 1) * size), scaled, 0.0).astype(bf16)
            first = jnp.exp(jnp.where(causal_t, row[:, :half] - col[:half], BLOCKED))
            right = jnp.exp(row[:, half:] - col[:half])
            last = jnp.exp(jnp.where(causal_t, row[:, half:] - col[half:], BLOCKED))
            top = mm(
                jnp.concatenate(
                    [
                        (first * scores_t[:half, :half]).astype(bf16),
                        (right * scores_t[:half, half:]).astype(bf16),
                    ],
                    axis=1,
                ),
                dmixed_b,
            )
            bottom = mm((last * scores_t[half:, half:]).astype(bf16), dmixed_b[half:])
            part = jnp.concatenate([top, bottom], axis=0)
            dscaled = part if dscaled is None else jnp.where(lane >= k * size, part, dscaled)
            dscores[:half, :half] += mm_nt(own[:half], dmixed_b[:half]) * first
            dscores[:half, half:] += mm_nt(own[:half], dmixed_b[half:]) * right
            dscores[half:, half:] += mm_nt(own[half:], dmixed_b[half:]) * last
        in_wide = mm_split(decay_in, spread)
        out_wide = mm_split(decay_out, spread)
        dheld = dstate[:, cols]
        dheld_b = dheld.astype(bf16)
        dstate_b[:, cols] = dheld_b
        dlate = out_wide * mm(keys, dheld_b)
        dscaled = dscaled + dlate
        rounded = scaled_b.astype(f32)
        dcumul = dcumul + mm_split(dmixed_b.astype(f32) * scanned - rounded * dscaled, gather)
        dsteps = dsteps + mm_split(inner * dscaled, gather)
        final_wide = in_wide[count - 1 : count, :]
        finals[0:1, cols] = jnp.sum(rounded * dlate, axis=0, keepdims=True) + final_wide * jnp.sum(
            dheld * states_ref[0, :, cols], axis=0, keepdims=True
        )
        dinner = dscaled * steps_wide + skip_ref[:, cols] * dmixed
        ext[0:count, cols] = dinner * (sig * (1.0 + conv * (1.0 - sig)))
        in_b = (in_wide * dmixed).astype(bf16)
        in_rows[:, cols] = in_b
        out_rows[:, cols] = (out_wide * scaled).astype(bf16)
        dstate[:, cols] = final_wide * dheld + mm(queries_t, in_b)

    pairs = dscores[...]
    dkeys = mm(pairs.astype(bf16), queries) + mm_nt(out_rows[...], dstate_b[...])
    dqueries = mm(pairs.T.astype(bf16), keys) + mm_nt(in_rows[...], states_ref[0].astype(bf16))
    ext[0:count, key_cols] = dkeys * (key_sig * (1.0 + key_pre * (1.0 - key_sig)))
    ext[0:count, query_cols] = dqueries * (query_sig * (1.0 + query_pre * (1.0 - query_sig)))

    for start in range(0, conv_width, LANES):
        cols = slice(start, start + LANES)
        pre = pre_ref[:, width + start : width + start + LANES]
        total = None
        for j in range(taps):
            moved = ext[taps - 1 - j : taps - 1 - j + count, cols]
            term = taps_ref[j : j + 1, cols] * moved
            total = term if total is None else total + term
            taps_grad_ref[j : j + 1, cols] += jnp.sum(pre * moved, axis=0, keepdims=True)
        taps_grad_ref[taps : taps + 1, cols] += jnp.sum(ext[0:count, cols], axis=0, keepdims=True)
        dpre_ref[:, width + start : width + start + LANES] = total.astype(bf16)
        ext[count : count + CARRY, cols] = ext[0:CARRY, cols]

    final_row = mm_split(jnp.broadcast_to(finals[0:1, :], (CARRY, width)), gather_ref[...])[0:1]
    suffix = 1.0 - tri_lower(count).astype(f32) + jnp.where(
        lax.broadcasted_iota(jnp.int32, (count, count), 0)
        == lax.broadcasted_iota(jnp.int32, (count, count), 1),
        1.0,
        0.0,
    )
    dlogs = mm_exact(suffix, dcumul) + final_row
    dshifted = (dsteps + dlogs * heads_ref[0:1, :]) * sigmoid(shifted)
    dpre_ref[:, width + conv_width :] = dshifted.astype(bf16)
    heads_grad_ref[0:1, :] += jnp.sum(dlogs * logs, axis=0, keepdims=True)
    heads_grad_ref[1:2, :] += jnp.sum(dshifted, axis=0, keepdims=True)

    @pl.when(closing)
    def _():
        own_ref[...] = exchange.finish()
        skips = jnp.broadcast_to(wide_grad_ref[1:2, :], (CARRY, width))
        heads_grad_ref[2:3, :] = mm_split(skips, gather_ref[...])[0:1]


def whole(shape):
    return pl.BlockSpec(shape, lambda s, i: (0,) * len(shape))


def run_forward(pre, taps, heads, skip, spread, seqs, count, size):
    rows, cat = pre.shape
    width = skip.shape[1]
    conv_width = taps.shape[1]
    state_size = (conv_width - width) // 2
    blocks = rows // seqs // count

    def block(cols):
        return pl.BlockSpec((count, cols), lambda s, i: (s * blocks + i, 0))

    return pl.pallas_call(
        functools.partial(forward_kernel, width, size),
        grid=(seqs, blocks),
        in_specs=[block(cat), whole(taps.shape), whole(heads.shape), whole(skip.shape), whole(spread.shape)],
        out_specs=[
            block(width), block(conv_width), block(width),
            pl.BlockSpec((1, state_size, width), lambda s, i: (s * blocks + i, 0, 0)),
        ],
        out_shape=[
            jax.ShapeDtypeStruct((rows, width), f32),
            jax.ShapeDtypeStruct((rows, conv_width), f32),
            jax.ShapeDtypeStruct((rows, width), f32),
            jax.ShapeDtypeStruct((seqs * blocks, state_size, width), f32),
        ],
        scratch_shapes=[
            pltpu.VMEM((count + CARRY, conv_width), f32),
            pltpu.VMEM((state_size, width), f32),
            pltpu.VMEM((count, conv_width), f32),
        ],
        cost_estimate=pl.CostEstimate(
            flops=rows * width * count * 4, bytes_accessed=rows * (cat + 4 * width) * 4, transcendentals=rows * count * 12
        ),
        name="mixer_forward",
    )(pre, taps, heads, skip, spread)


def run_backward(pre, conv, scanned, dnormed, token, states, taps, heads, skip, gain, spread, gather, terms, n, seqs, count, size):
    rows, cat = pre.shape
    width = skip.shape[1]
    conv_width = taps.shape[1]
    state_size = (conv_width - width) // 2
    blocks = rows // seqs // count

    def block(cols):
        return pl.BlockSpec((count, cols), lambda s, i: (s * blocks + blocks - 1 - i, 0))

    return pl.pallas_call(
        functools.partial(backward_kernel, n, blocks, width, size),
        grid=(seqs, blocks),
        in_specs=[
            block(cat), block(conv_width), block(width), block(width), block(2),
            pl.BlockSpec((1, state_size, width), lambda s, i: (s * blocks + blocks - 1 - i, 0, 0)),
            whole(taps.shape), whole(heads.shape), whole(skip.shape), whole(gain.shape),
            whole(spread.shape), whole(gather.shape),
            pl.BlockSpec(memory_space=pl.ANY),
        ],
        out_specs=[
            block(cat), whole((8, conv_width)), whole((8, width)), whole((8, LANES)),
            whole((terms.shape[0] // n, terms.shape[1])),
        ],
        out_shape=[
            jax.ShapeDtypeStruct((rows, cat), bf16),
            jax.ShapeDtypeStruct((8, conv_width), f32),
            jax.ShapeDtypeStruct((8, width), f32),
            jax.ShapeDtypeStruct((8, LANES), f32),
            jax.ShapeDtypeStruct((terms.shape[0] // n, terms.shape[1]), f32),
        ],
        scratch_shapes=[
            pltpu.VMEM((count + CARRY, conv_width), f32),
            pltpu.VMEM((state_size, width), f32),
            pltpu.VMEM((count, count), f32),
            pltpu.VMEM((count, width), bf16),
            pltpu.VMEM((count, width), bf16),
            pltpu.VMEM((state_size, width), bf16),
            pltpu.VMEM((8, width), f32),
        ]
        + Exchange.scratch(n, terms.shape[0] // n, terms.shape[1]),
        compiler_params=pltpu.CompilerParams(
            collective_id=2, has_side_effects=True, vmem_limit_bytes=56 * 1024 * 1024
        ),
        cost_estimate=pl.CostEstimate(
            flops=rows * width * count * 8, bytes_accessed=rows * (2 * cat + 4 * width) * 4, transcendentals=rows * count * 12
        ),
        name="mixer_backward",
    )(pre, conv, scanned, dnormed, token, states, taps, heads, skip, gain, spread, gather, terms)


def adam_step(param, first, second_moment, grad, rate):
    first_new = beta_first * first + (1.0 - beta_first) * grad
    second_new = beta_second * second_moment + (1.0 - beta_second) * grad * grad
    first_hat = first_new / (1.0 - beta_first**step_count)
    second_hat = second_new / (1.0 - beta_second**step_count)
    moved = param - rate * (first_hat / (jnp.sqrt(second_hat) + adam_eps) + decay_rate * param)
    return (moved, first_new, second_new)


def flip_step(values):
    return tuple(value.T if k == 2 else value for k, value in enumerate(values))


def body(hidden, cotangent, *arrays):
    params, firsts, seconds = arrays[:9], arrays[9:18], arrays[18:27]
    (
        input_gain,
        inner_weight,
        step_weight,
        state_weight,
        inner_taps,
        state_taps,
        head_params,
        gated_gain,
        output_matrix,
    ) = params
    _, seqs, features = hidden.shape
    wide = inner_taps.shape[1]
    heads = head_params.shape[1]
    size = wide // heads
    states = state_taps.shape[1]
    shards = lax.axis_size("tensor")
    inner_total = wide * shards

    base = hidden.astype(f32)
    rstd = lax.rsqrt(jnp.mean(base * base, -1, keepdims=True) + norm_eps)
    normed = base * rstd
    normed_in = (normed * input_gain).astype(bf16)

    def by_sequence(values):
        return values.transpose(1, 0, 2).reshape(values.shape[0] * seqs, values.shape[2])

    def by_position(values):
        return values.reshape(seqs, values.shape[0] // seqs, values.shape[1]).transpose(1, 0, 2)

    state_rows = gather_tensor(state_weight.astype(bf16), shards).reshape(-1, states)
    full_in = lax.all_gather(normed_in, "tensor", axis=0, tiled=True)
    weights_own = jnp.concatenate(
        [
            inner_weight[0].astype(bf16),
            inner_weight[1].astype(bf16),
            state_rows,
            jnp.pad(step_weight.astype(bf16), ((0, 0), (0, LANES - heads))),
        ],
        axis=1,
    )
    replicas = lax.axis_size("dp")
    gathered = gather_dp(
        jnp.concatenate([weights_own, output_matrix.astype(bf16).T], axis=1), replicas
    )
    cat = weights_own.shape[1]
    weights = gathered[:, :cat]
    output_t = gathered[:, cat:]
    full_cot = lax.all_gather(cotangent, "tensor", axis=0, tiled=True)
    flat_in = by_sequence(full_in)
    flat_cot = by_sequence(full_cot)

    taps = jnp.concatenate([inner_taps, state_taps], axis=1)
    head_rows = jnp.pad(
        jnp.stack([-jnp.exp(head_params[0]), head_params[1]]), ((0, 0), (0, LANES - heads))
    )
    skip = jnp.repeat(head_params[2], size)[None]
    gain = gated_gain[None]
    spread = (jnp.arange(LANES)[:, None] == jnp.arange(wide)[None] // size).astype(bf16)
    gather = (jnp.arange(wide)[:, None] // size == jnp.arange(LANES)[None]).astype(bf16)

    pre = mm(flat_in, weights)
    scanned, conv, gated, chunk_states = run_forward(
        pre, taps, head_rows, skip, spread, seqs, GROUP, size
    )
    d_normed = mm(flat_cot, output_t)
    sums = sum_tensor(
        jnp.stack([jnp.sum(gated * gated, -1), jnp.sum(d_normed * gain * gated, -1)]), shards
    )
    scale_row = lax.rsqrt(sums[0] / inner_total + norm_eps)
    token = jnp.stack([scale_row, scale_row**3 * (sums[1] / inner_total)], axis=1)
    scale = token[:, 0:1]
    normed_out = (gated * scale * gain).astype(bf16)
    branch_part = by_position(mm_nt(normed_out, output_t)).astype(bf16)
    branch_part, d_normed = lax.optimization_barrier((branch_part, d_normed))
    branch = lax.psum_scatter(branch_part, "tensor", scatter_dimension=0, tiled=True)
    output_terms = contract_first(flat_cot, normed_out)

    d_pre, taps_grad, wide_grad, head_grad, grad_output_t = run_backward(
        pre, conv, scanned, d_normed, token, chunk_states, taps, head_rows, skip, gain,
        spread, gather, output_terms, replicas, seqs, GROUP, size,
    )
    d_in_part = mm_nt(d_pre, weights)
    d_in = lax.psum_scatter(by_position(d_in_part.astype(bf16)), "tensor", scatter_dimension=0, tiled=True).astype(f32)
    grad_gain_rows = jnp.sum(d_in_part * flat_in.astype(f32), axis=0) / input_gain
    gain_cols = -(-features // (8 * LANES)) * LANES
    small = jnp.concatenate(
        [
            taps_grad,
            wide_grad,
            head_grad,
            jnp.pad(grad_gain_rows, (0, 8 * gain_cols - features)).reshape(8, gain_cols),
        ],
        axis=1,
    )
    grad_inner, step_sums, grad_state, grad_taps, grad_wide, head_sums, grad_state_taps, gain_sums = sum_dp(
        flat_in.T, d_pre, small, replicas, shards, wide, states, inner_taps.shape[0]
    )
    grad_output = grad_output_t.T

    result = (base + branch.astype(f32)).astype(bf16)
    d_hat = d_in * input_gain
    gradient_hidden = cotangent.astype(f32) + rstd * (
        d_hat - normed * jnp.mean(d_hat * normed, -1, keepdims=True)
    )
    grads = (
        gain_sums.reshape(-1)[:features],
        grad_inner,
        step_sums[:heads],
        grad_state,
        grad_taps,
        grad_state_taps,
        head_sums[:3, :heads],
        grad_wide[0],
        grad_output,
    )
    stepped = [
        adam_step(param, first, second_moment, grad, rate)
        for param, first, second_moment, grad, rate in zip(
            flip_step(params), flip_step(firsts), flip_step(seconds), grads, rates
        )
    ]
    grads = flip_step(grads)
    stepped = [entry if k != 2 else tuple(value.T for value in entry) for k, entry in enumerate(stepped)]
    moved = [entry[0] for entry in stepped]
    first_new = [entry[1] for entry in stepped]
    second_new = [entry[2] for entry in stepped]
    return (result, gradient_hidden, *grads, *moved, *first_new, *second_new)


def contract_first(left, right):
    return lax.dot_general(left, right, (((0,), (0,)), ((), ())), preferred_element_type=f32)


def solution(mesh):
    weights = (
        P(),
        P(None, "dp", "tensor"),
        P("dp", "tensor"),
        P(("dp", "tensor"), None),
        P(None, "tensor"),
        P(),
        P(None, "tensor"),
        P("tensor"),
        P("tensor", "dp"),
    )
    rows = P("tensor", "dp", None)

    return jax.shard_map(
        body,
        mesh=mesh,
        in_specs=(rows, rows) + weights * 3,
        out_specs=(rows, rows) + weights * 4,
        check_vma=False,
    )
```
